32 devices in a mesh: section: 4 (over y, x), dp: 2 (over core), head: 4 (over z).
Axes of the slice: x: 2, y: 2, z: 4, core: 2. Of those that a mesh axis runs over, the one named last changes fastest.
Arguments:
- queries: bfloat16 [2, 4, 256, 12288], P(None, 'section', 'dp', 'head'), may hold values from -40 to 40
- latents: bfloat16 [2, 4, 256, 576], P(None, 'section', 'dp'), may hold values from -6 to 6
- out_grad: bfloat16 [2, 4, 256, 8192], P(None, 'section', 'dp', 'head'), may hold values from -6 to 6
- segment_ids: int32 [2, 4, 256], P(None, 'section', 'dp'), may hold values from 0 to 7, never falling along the last dimension, each value on 1 to 128 neighbouring positions
- up_weight: bfloat16 [2, 4, 512, 16384], P(None, 'section', None, 'head'), may hold values from -0.25 to 0.25
Outputs:
- query_grad: bfloat16 [2, 4, 256, 12288], P(None, 'section', 'dp', 'head')
- latent_grad: bfloat16 [2, 4, 256, 576], P(None, 'section', ('dp', 'head'))
- weight_grad: float32 [4, 512, 16384], P('section', 'dp', 'head')
The draws below stay inside these ranges and needn't reach their ends.
All inputs are finite; a program needn't handle non-finite values.
Results may differ from the reference program's by a relative error of at most 0.017.
Values may be sent and summed in bfloat16 or wider, within the bound.
A program may use at most 64 MiB of HBM per device.

```python
import math
import jax
import jax.numpy as jnp
import numpy as np
from jax import lax

LATENT = 512
ROPE = 64
NOPE = 128
VDIM = 128
HEADS = 64
TOK = 128
SECTIONS = 4
ROWS = 256
N_DP = 2


def joint_draw(key):
    base = jax.random.fold_in(key, 11)
    first, second = jax.random.split(base, 2)
    query_shape = (2, SECTIONS, ROWS, HEADS, NOPE + ROPE)
    latent_shape = (2, SECTIONS, ROWS, LATENT + ROPE)
    latent_vals = jnp.clip(jax.random.normal(first, latent_shape, jnp.float32), -6.0, 6.0)
    query_vals = jnp.clip(jax.random.normal(second, query_shape, jnp.float32), -6.0, 6.0)
    return (query_vals.reshape(2, SECTIONS, ROWS, HEADS * (NOPE + ROPE)), latent_vals)


def draw_queries(key, part):
    return joint_draw(key)[0].astype(jnp.bfloat16)


def draw_latents(key, part):
    return joint_draw(key)[1].astype(jnp.bfloat16)


def steps_of(own_key, shape, cuts, smallest, high):
    def one(position, shards_of):
        heights = jax.random.uniform(jax.random.fold_in(jax.random.fold_in(own_key, 6), position), (shards_of,), jnp.float32, smallest / len(cuts), high / len(cuts))
        return jnp.repeat(jnp.exp(heights), shape[position] // shards_of).reshape((-1,) + (1,) * (len(shape) - position - 1))

    loudness = one(*cuts[0])
    for cut in cuts[1:]:
        loudness = loudness * one(*cut)
    return loudness


def profile(number_of, total, limit, lean):
    portions = [(1 << 20) // math.isqrt(rank ** lean) + 1 for rank in range(2, number_of + 1)]
    spare, holding = total - limit - (number_of - 1), [1] * (number_of - 1)
    while spare > 0:
        candidates = [i for i in range(number_of - 1) if holding[i] < limit]
        whole, left = sum([portions[i] for i in candidates]), spare
        for i in candidates:
            more = min(limit - holding[i], max(1, left * portions[i] // whole), spare)
            holding[i] = holding[i] + more
            spare = spare - more
    return np.array([limit] + holding)


def uneven(rng, amount, total, bound, skew):
    if amount == 2:
        one = jax.random.randint(rng, (), max(1, total - bound), min(bound, total - 1) + 1)
        return jnp.stack([one, total - one])
    sizes = jnp.asarray(profile(amount, total, bound, skew), jnp.int32)
    twos = (amount - 1) // 2
    donor, receiver = sizes[1:1 + 2 * twos:2], sizes[2:2 + 2 * twos:2]
    slack = jnp.minimum(donor - 1, bound - receiver)
    moved = jax.random.randint(jax.random.fold_in(rng, 1), (twos,), 0, 1 << 20) % (slack + 1)
    sizes = sizes.at[1:1 + 2 * twos:2].set(donor - moved).at[2:2 + 2 * twos:2].set(receiver + moved)
    return sizes[jax.random.permutation(jax.random.fold_in(rng, 2), amount)]


def normal_values(rng, shape, width, reach, cuts=(), held_as=jnp.bfloat16):
    gain = steps_of(rng, shape, cuts, -0.22, 0.18) if cuts else 1.0
    drawn = jax.random.normal(rng, shape, jnp.float32) * width * gain
    return jnp.minimum(jnp.maximum(drawn, -reach), reach).astype(held_as)


def setup_inputs(seed: int = 0) -> dict:
    seeds = jax.random.split(jax.random.key(seed), 6)
    return {
        "queries": draw_queries(jax.random.fold_in(seeds[5], 71), 0),
        "latents": draw_latents(jax.random.fold_in(seeds[5], 71), 0),
        "out_grad": normal_values(seeds[2], (2, SECTIONS, ROWS, HEADS * VDIM), 1.0, 6.0, ((1, 4), (2, 2), (3, 4))),
        "segment_ids": jax.vmap(lambda own: jnp.searchsorted(jnp.cumsum(uneven(own, 4 * N_DP, ROWS, TOK, 1)), jnp.arange(ROWS), side="right"))(jax.random.split(seeds[3], 2 * SECTIONS)).reshape((2, SECTIONS, ROWS)).astype(jnp.int32),
        "up_weight": normal_values(seeds[4], (2, SECTIONS, LATENT, HEADS * (NOPE + VDIM)), LATENT ** -0.5, 0.25, ((1, 4), (3, 4))),
    }


def micro_grads(queries, latents, out_grad, segment_ids, weight):
    tokens = queries.shape[0]
    latent_plain = latents[:, :LATENT]
    key_rope = latents[:, LATENT:].astype(jnp.float32)
    kv_full = jnp.dot(latent_plain, weight, preferred_element_type=jnp.float32).astype(jnp.bfloat16)
    kv_full = kv_full.astype(jnp.float32).reshape(tokens, HEADS, NOPE + VDIM)
    key_plain = kv_full[..., :NOPE]
    values = kv_full[..., NOPE:]
    query_heads = queries.astype(jnp.float32).reshape(tokens, HEADS, NOPE + ROPE)
    query_plain = query_heads[..., :NOPE]
    query_rope = query_heads[..., NOPE:]
    out_heads = out_grad.astype(jnp.float32).reshape(tokens, HEADS, VDIM)
    scale = (NOPE + ROPE) ** -0.5
    scores = (jnp.einsum('thd,shd->hts', query_plain, key_plain) + jnp.einsum('thd,sd->hts', query_rope, key_rope)) * scale
    positions = jnp.arange(tokens)
    allowed = (positions[:, None] >= positions[None, :]) & (segment_ids[:, None] == segment_ids[None, :])
    scores = jnp.where(allowed[None], scores, jnp.float32(-1e30))
    probs = jax.nn.softmax(scores, axis=-1)
    grad_probs = jnp.einsum('thd,shd->hts', out_heads, values)
    delta = jnp.sum(probs * grad_probs, axis=-1, keepdims=True)
    score_grad = (probs * (grad_probs - delta) * scale).astype(jnp.bfloat16).astype(jnp.float32)
    probs_low = probs.astype(jnp.bfloat16).astype(jnp.float32)
    value_grad = jnp.einsum('hts,thd->shd', probs_low, out_heads)
    key_grad = jnp.einsum('hts,thd->shd', score_grad, query_plain)
    rope_grad = jnp.einsum('hts,thd->sd', score_grad, query_rope)
    grad_plain = jnp.einsum('hts,shd->thd', score_grad, key_plain)
    grad_rope = jnp.einsum('hts,sd->thd', score_grad, key_rope)
    query_grad = jnp.concatenate([grad_plain, grad_rope], -1).reshape(tokens, -1).astype(jnp.bfloat16)
    kv_grad = jnp.concatenate([key_grad, value_grad], -1).reshape(tokens, -1).astype(jnp.bfloat16)
    latent_part = jnp.dot(kv_grad, weight.T, preferred_element_type=jnp.float32)
    local_latent = jnp.concatenate([latent_part, rope_grad], 1).astype(jnp.bfloat16)
    partial_value = jnp.dot(latent_plain.T, kv_grad, preferred_element_type=jnp.float32)
    return query_grad, local_latent, partial_value


def direction_grads(queries, latents, out_grad, segment_ids, weights):
    sections = queries.shape[0]
    query_items = queries.reshape(sections, N_DP, TOK, -1)
    latent_items = latents.reshape(sections, N_DP, TOK, -1)
    out_items = out_grad.reshape(sections, N_DP, TOK, -1)
    segment_items = segment_ids.reshape(sections, N_DP, TOK)

    def one_section(items):
        q_section, l_section, o_section, s_section, weight = items

        def step(total, inner):
            query_grad, local_latent, partial_value = micro_grads(inner[0], inner[1], inner[2], inner[3], weight)
            rounded = lax.optimization_barrier(partial_value.astype(jnp.bfloat16)).astype(jnp.float32)
            return total + rounded, (query_grad, local_latent)

        start = jnp.zeros((LATENT, HEADS * (NOPE + VDIM)), jnp.float32)
        total, (query_grads, latent_grads) = lax.scan(step, start, (q_section, l_section, o_section, s_section))
        return query_grads, latent_grads, total

    query_grads, latent_grads, totals = lax.map(one_section, (query_items, latent_items, out_items, segment_items, weights))
    return query_grads.reshape(sections, N_DP * TOK, -1), latent_grads.reshape(sections, N_DP * TOK, -1), totals


def reference(queries, latents, out_grad, segment_ids, up_weight):
    q_fwd, l_fwd, w_fwd = direction_grads(queries[0], latents[0], out_grad[0], segment_ids[0], up_weight[0])
    q_rev, l_rev, w_rev = direction_grads(queries[1], latents[1], out_grad[1], segment_ids[1], up_weight[1])
    q_fwd = jnp.concatenate([q_fwd[1:], jnp.zeros_like(q_fwd[:1])], 0)
    l_fwd = jnp.concatenate([l_fwd[1:], jnp.zeros_like(l_fwd[:1])], 0)
    q_rev = jnp.concatenate([jnp.zeros_like(q_rev[:1]), q_rev[:-1]], 0)
    l_rev = jnp.concatenate([jnp.zeros_like(l_rev[:1]), l_rev[:-1]], 0)
    query_grad = jnp.stack([q_fwd, q_rev], 0)
    latent_grad = jnp.stack([l_fwd, l_rev], 0)
    weight_grad = w_fwd + w_rev[::-1]
    return query_grad, latent_grad, weight_grad
```

```python
import functools

import jax
import jax.numpy as jnp
from jax import lax
from jax.experimental import pallas as pl
from jax.experimental.pallas import tpu as pltpu
from jax.sharding import PartitionSpec as P

ROPE = 64
NOPE = 128
VDIM = 128
QDIM = NOPE + ROPE
KVDIM = NOPE + VDIM
GROUP = 4
FWD, REV = 0, 1
MESH = pl.DeviceIdType.MESH


def dot(a, b, contract):
    return lax.dot_general(a, b, ((contract[:1], contract[1:]), ((), ())), preferred_element_type=jnp.float32)


def relay_kernel(
    sizes,
    queries, latents_t, out_grad, segments, weight,
    query_grad, latent_grad, weight_grad,
    q_buf, lt_buf, o_buf, w_buf, lat, rope, kv_rev, kv_all, lt_all, q_out, relay_buf, zeros, small_zeros,
    local, pieces, sums, rope_sum, w_out,
    q_in, lt_in, o_in, w_in, w_put, z_put,
    kr_send, kr_recv, kf_send, kf_recv, kx_send, kx_recv, lr_send, lr_recv, lf_send, lf_recv,
    qs_send, qs_recv, rl_send, rl_recv, rf_send, hp_send, hp_recv, ls_send, ls_recv,
):
    n_section, n_dp, n_head, heads, groups = sizes
    me, my_dp, my_head = lax.axis_index("section"), lax.axis_index("dp"), lax.axis_index("head")
    mirror = n_section - 1 - me
    tokens = queries.shape[2]
    latent = weight.shape[2]
    rows = latent // n_dp
    mine = tokens // n_head
    kw, qw, ow = heads * KVDIM, heads * QDIM, heads * VDIM
    half = q_out.shape[2] // 2
    relayed = n_section == 4
    scale = QDIM ** (-0.5)

    def remote(src, dst, send, recv, **where):
        return pltpu.make_async_remote_copy(
            src_ref=src, dst_ref=dst, send_sem=send, recv_sem=recv, device_id=where, device_id_type=MESH
        )

    def dp_peer(k):
        return lax.rem(my_dp + k, n_dp)

    def dp_from(k):
        return lax.rem(my_dp + n_dp - k, n_dp)

    def head_peer(k):
        return lax.rem(my_head + k, n_head)

    def load_weight(r, g):
        cols = pl.ds(pl.multiple_of(g * kw, 128), kw)
        return pltpu.make_async_copy(weight.at[r, 0, :, cols], w_buf.at[r, g], w_in.at[r, g])

    def load_latents(r):
        return pltpu.make_async_copy(latents_t.at[r, 0], lt_buf.at[r], lt_in.at[r])

    def load_queries(r):
        return pltpu.make_async_copy(queries.at[r, 0], q_buf.at[r], q_in.at[r])

    def load_out(r):
        return pltpu.make_async_copy(out_grad.at[r, 0], o_buf.at[r], o_in.at[r])

    barrier = pltpu.get_barrier_semaphore()
    for k in range(1, n_section):
        pl.semaphore_signal(barrier, 1, device_id={"section": lax.rem(me + k, n_section)}, device_id_type=MESH)
    for k in range(1, n_dp):
        pl.semaphore_signal(barrier, 1, device_id={"dp": dp_peer(k)}, device_id_type=MESH)
        pl.semaphore_signal(barrier, 1, device_id={"section": mirror, "dp": dp_peer(k)}, device_id_type=MESH)
    for k in range(1, n_head):
        pl.semaphore_signal(barrier, 1, device_id={"head": head_peer(k)}, device_id_type=MESH)

    for r in (REV, FWD):
        load_latents(r).start()
        load_weight(r, 0).start()
        load_queries(r).start()
        load_out(r).start()

        @pl.loop(1, groups)
        def _(g):
            load_weight(r, g).start()

    zeros[...] = jnp.zeros_like(zeros)
    small_zeros[...] = jnp.zeros_like(small_zeros)
    for r in (REV, FWD):
        load_latents(r).wait()
        plain = lt_buf[r, :latent, :].astype(jnp.float32)
        lat[r] = jnp.transpose(plain).astype(jnp.bfloat16)
        rope[r] = jnp.transpose(lt_buf[r, latent:, :].astype(jnp.float32)).astype(jnp.bfloat16)
    rope_sum[...] = jnp.zeros_like(rope_sum)

    pl.semaphore_wait(barrier, n_section - 1 + 2 * (n_dp - 1) + n_head - 1)

    def latent_rev(k):
        to = dp_peer(k)
        block = pl.ds(pl.multiple_of(to * rows, rows), rows)
        return remote(
            lt_buf.at[REV, block], lt_all.at[n_dp + my_dp], lr_send.at[k], lr_recv.at[k], section=mirror, dp=to
        )

    def latent_fwd(k):
        to = dp_peer(k)
        block = pl.ds(pl.multiple_of(to * rows, rows), rows)
        return remote(lt_buf.at[FWD, block], lt_all.at[my_dp], lf_send.at[k], lf_recv.at[k], dp=to)

    for k in range(n_dp):
        latent_rev(k).start()
    for k in range(1, n_dp):
        latent_fwd(k).start()
    lt_all[my_dp] = lt_buf[FWD, pl.ds(pl.multiple_of(my_dp * rows, rows), rows), :]

    def fill(r):
        quarter = zeros.shape[1]
        return [
            pltpu.make_async_copy(zeros, query_grad.at[r, 0, :, pl.ds(c * quarter, quarter)], z_put.at[c])
            for c in range(q_out.shape[2] // quarter)
        ] + [pltpu.make_async_copy(small_zeros, latent_grad.at[r, 0], z_put.at[q_out.shape[2] // quarter])]

    def slot(piece):
        return pl.ds(pl.multiple_of(piece * tokens, tokens), tokens)

    def kv_to_mirror(g):
        return remote(kv_rev.at[g], kv_all.at[g, slot(n_dp + my_dp)], kr_send.at[g], kr_recv.at[g], section=mirror)

    def kv_to_peer(g, k):
        ref = kv_all.at[g, slot(my_dp)]
        return remote(ref, ref, kf_send.at[g, k], kf_recv.at[g, k], dp=dp_peer(k))

    def kv_passed_on(g, k):
        ref = kv_all.at[g, slot(n_dp + my_dp)]
        return remote(ref, ref, kx_send.at[g, k], kx_recv.at[g, k], dp=dp_peer(k))

    def compute(r, g, allowed):
        load_weight(r, g).wait()
        kv = dot(lat[r], w_buf[r, g], (1, 0)).astype(jnp.bfloat16)
        query_block = q_buf[r, :, pl.ds(pl.multiple_of(g * qw, 128), qw)]
        out_block = o_buf[r, :, pl.ds(pl.multiple_of(g * ow, 128), ow)]
        key_rope = rope[r]
        query_parts, kv_parts = [], []
        total = rope_sum[r]
        for h in range(heads):
            key = jnp.concatenate([kv[:, h * KVDIM : h * KVDIM + NOPE], key_rope], 1)
            value = kv[:, h * KVDIM + NOPE : (h + 1) * KVDIM]
            query = query_block[:, h * QDIM : (h + 1) * QDIM]
            out = out_block[:, h * VDIM : (h + 1) * VDIM]
            scores = jnp.where(allowed, dot(key, query, (1, 1)) * scale, jnp.float32(-1e30))
            powers = jnp.exp(scores - jnp.max(scores, axis=0, keepdims=True))
            probs = powers * (1.0 / jnp.sum(powers, axis=0, keepdims=True))
            grad_probs = dot(value, out, (1, 1))
            delta = jnp.sum(probs * grad_probs, axis=0, keepdims=True)
            score_grad = (probs * (grad_probs - delta) * scale).astype(jnp.bfloat16)
            value_grad = dot(probs.astype(jnp.bfloat16), out, (1, 0))
            key_grad = dot(score_grad, query, (1, 0))
            total += key_grad[:, NOPE:]
            query_parts.append(dot(score_grad, key, (0, 0)))
            kv_parts += [key_grad[:, :NOPE].astype(jnp.bfloat16), value_grad.astype(jnp.bfloat16)]
        rope_sum[r] = total
        q_out[r, :, pl.ds(pl.multiple_of(g * qw, 128), qw)] = jnp.concatenate(query_parts, 1).astype(jnp.bfloat16)
        kv_out = jnp.concatenate(kv_parts, 1)
        if r == REV:
            kv_rev[g] = kv_out
            kv_to_mirror(g).start()
        else:
            kv_all[g, slot(my_dp), :] = kv_out
            for k in range(1, n_dp):
                kv_to_peer(g, k).start()

    def cut(c):
        return pl.ds(c * half, half)

    def query_copy(r, c):
        to = me - 1 if r == FWD else me + 1
        return remote(
            q_out.at[r, :, cut(c)], query_grad.at[r, 0, :, cut(c)], qs_send.at[r, c], qs_recv.at[r, c], section=to
        )

    def to_relay(r):
        return remote(q_out.at[r, :, cut(0)], relay_buf, rl_send.at[r], rl_recv, section=me - 2 if r == FWD else me + 2)

    def from_relay(r):
        to = me + 1 if r == FWD else me - 1
        return remote(relay_buf, query_grad.at[r, 0, :, cut(0)], rf_send, qs_recv.at[r, 0], section=to)

    sends = {FWD: me > 0, REV: me < n_section - 1}
    receives = {FWD: me < n_section - 1, REV: me > 0}
    relays_out = {FWD: me == 2, REV: me == 1}
    relays_for = {FWD: me == 0, REV: me == 3}

    def send_queries(r):
        if relayed:

            @pl.when(relays_out[r])
            def _():
                to_relay(r).start()

            @pl.when(sends[r] & jnp.logical_not(relays_out[r]))
            def _():
                query_copy(r, 0).start()
        else:

            @pl.when(sends[r])
            def _():
                query_copy(r, 0).start()

        @pl.when(sends[r])
        def _():
            query_copy(r, 1).start()

    def head_copy(r, k):
        to = head_peer(k)
        return remote(
            local.at[r, pl.ds(pl.multiple_of(to * mine, mine), mine)],
            pieces.at[r, k - 1],
            hp_send.at[r, k],
            hp_recv.at[r, k],
            head=to,
        )

    def latent_out(r):
        to = me - 1 if r == FWD else me + 1
        return remote(sums.at[r], latent_grad.at[r, 0], ls_send.at[r], ls_recv.at[r], section=to)

    for r in (REV, FWD):
        load_queries(r).wait()
        load_out(r).wait()
        seg = jnp.broadcast_to(segments[r], (tokens, tokens))
        keys = lax.broadcasted_iota(jnp.int32, (tokens, tokens), 0)
        at = lax.broadcasted_iota(jnp.int32, (tokens, tokens), 1)
        allowed = (at >= keys) & (seg == jnp.transpose(seg))

        @pl.loop(0, groups)
        def _(g):
            compute(r, g, allowed)

        send_queries(r)

    if relayed:
        for r in (REV, FWD):

            @pl.when(relays_for[r])
            def _():
                to_relay(r).wait_recv()
                from_relay(r).start()

    for r in (REV, FWD):

        def add(g, total):
            block = kv_rev[g] if r == REV else kv_all[g, slot(my_dp), :]
            return total + dot(block, w_buf[r, g], (1, 1))

        total = lax.fori_loop(0, groups, add, jnp.zeros((tokens, latent), jnp.float32))
        local[r] = jnp.concatenate([total, rope_sum[r]], 1).astype(jnp.bfloat16)
        for k in range(1, n_head):
            head_copy(r, k).start()

    for r in (REV, FWD):
        total = local[r, pl.ds(pl.multiple_of(my_head * mine, mine), mine), :].astype(jnp.float32)
        for k in range(1, n_head):
            head_copy(r, k).wait_recv()
            total += pieces[r, k - 1].astype(jnp.float32)
        sums[r] = total.astype(jnp.bfloat16)

        @pl.when(sends[r])
        def _():
            latent_out(r).start()

    for r in (FWD, REV):

        @pl.when(jnp.logical_not(receives[r]))
        def _():
            for copy in fill(r):
                copy.start()

    @pl.loop(0, groups)
    def _(g):
        kv_to_mirror(g).wait_recv()
        for k in range(1, n_dp):
            kv_passed_on(g, k).start()

    for k in range(n_dp):
        latent_rev(k).wait_recv()
    for k in range(1, n_dp):
        latent_fwd(k).wait_recv()
    latent_rows = jnp.concatenate([lt_all[p] for p in range(2 * n_dp)], 1)

    def put_weight(g):
        return pltpu.make_async_copy(
            w_out.at[g], weight_grad.at[0, :, pl.ds(pl.multiple_of(g * kw, 128), kw)], w_put.at[g]
        )

    @pl.loop(0, groups)
    def _(g):
        for k in range(1, n_dp):
            kv_to_peer(g, k).wait_recv()
            kv_passed_on(g, k).wait_recv()
        w_out[g] = dot(latent_rows, kv_all[g], (1, 0))
        put_weight(g).start()

    @pl.loop(0, groups)
    def _(g):
        put_weight(g).wait()
        kv_to_mirror(g).wait_send()
        for k in range(1, n_dp):
            kv_to_peer(g, k).wait_send()
            kv_passed_on(g, k).wait_send()

    for k in range(n_dp):
        latent_rev(k).wait_send()
    for k in range(1, n_dp):
        latent_fwd(k).wait_send()
    for r in (REV, FWD):
        for k in range(1, n_head):
            head_copy(r, k).wait_send()

        @pl.when(jnp.logical_not(receives[r]))
        def _():
            for copy in fill(r):
                copy.wait()

        if relayed:

            @pl.when(relays_out[r])
            def _():
                to_relay(r).wait_send()

            @pl.when(sends[r] & jnp.logical_not(relays_out[r]))
            def _():
                query_copy(r, 0).wait_send()

            @pl.when(relays_for[r])
            def _():
                from_relay(r).wait_send()
        else:

            @pl.when(sends[r])
            def _():
                query_copy(r, 0).wait_send()

        @pl.when(sends[r])
        def _():
            query_copy(r, 1).wait_send()
            latent_out(r).wait_send()

        @pl.when(receives[r])
        def _():
            query_copy(r, 0).wait_recv()
            query_copy(r, 1).wait_recv()
            latent_out(r).wait_recv()


def relay(mesh, queries, latents, out_grad, segment_ids, up_weight):
    n_section, n_dp, n_head = (mesh.shape[a] for a in ("section", "dp", "head"))
    tokens = queries.shape[2]
    latent, width = up_weight.shape[2:]
    features = latents.shape[3]
    heads_here = width // KVDIM
    heads = next(k for k in (GROUP, 2, heads_here) if heads_here % k == 0)
    groups = heads_here // heads
    rows, mine = latent // n_dp, tokens // n_head
    kw = heads * KVDIM
    q_width = heads_here * QDIM
    quarter = q_width // 4
    dma = pltpu.SemaphoreType.DMA
    bf16, f32 = jnp.bfloat16, jnp.float32
    anywhere, hbm = pl.BlockSpec(memory_space=pl.ANY), pl.BlockSpec(memory_space=pltpu.HBM)
    flops = 2 * (2 * tokens * width * latent * 2 + 2 * tokens * tokens * heads_here * 5 * KVDIM)
    return pl.pallas_call(
        functools.partial(relay_kernel, (n_section, n_dp, n_head, heads, groups)),
        in_specs=[hbm, hbm, hbm, pl.BlockSpec(memory_space=pltpu.VMEM), hbm],
        out_specs=[anywhere] * 3,
        out_shape=[
            jax.ShapeDtypeStruct((2, 1, tokens, q_width), bf16),
            jax.ShapeDtypeStruct((2, 1, mine, features), bf16),
            jax.ShapeDtypeStruct((1, rows, width), f32),
        ],
        scratch_shapes=[
            pltpu.VMEM((2, tokens, q_width), bf16),
            pltpu.VMEM((2, features, tokens), bf16),
            pltpu.VMEM((2, tokens, heads_here * VDIM), bf16),
            pltpu.VMEM((2, groups, latent, kw), bf16),
            pltpu.VMEM((2, tokens, latent), bf16),
            pltpu.VMEM((2, tokens, features - latent), bf16),
            pltpu.VMEM((groups, tokens, kw), bf16),
            pltpu.VMEM((groups, 2 * n_dp * tokens, kw), bf16),
            pltpu.VMEM((2 * n_dp, rows, tokens), bf16),
            pltpu.VMEM((2, tokens, q_width), bf16),
            pltpu.VMEM((tokens, q_width // 2), bf16),
            pltpu.VMEM((tokens, quarter), bf16),
            pltpu.VMEM((mine, features), bf16),
            pltpu.VMEM((2, tokens, features), bf16),
            pltpu.VMEM((2, n_head - 1, mine, features), bf16),
            pltpu.VMEM((2, mine, features), bf16),
            pltpu.VMEM((2, tokens, features - latent), f32),
            pltpu.VMEM((groups, rows, kw), f32),
            dma((2,)), dma((2,)), dma((2,)), dma((2, groups)), dma((groups,)), dma((5,)),
            dma((groups,)), dma((groups,)), dma((groups, n_dp)), dma((groups, n_dp)),
            dma((groups, n_dp)), dma((groups, n_dp)), dma((n_dp,)), dma((n_dp,)), dma((n_dp,)), dma((n_dp,)),
            dma((2, 2)), dma((2, 2)), dma((2,)), dma, dma, dma((2, n_head)), dma((2, n_head)), dma((2,)), dma((2,)),
        ],
        compiler_params=pltpu.CompilerParams(collective_id=0, has_side_effects=True, vmem_limit_bytes=44 << 20),
        cost_estimate=pl.CostEstimate(flops=flops, bytes_accessed=8 * latent * width, transcendentals=0),
        name="relay",
    )(queries, jnp.swapaxes(latents, 2, 3), out_grad, segment_ids, up_weight)


def solution(mesh):
    in_specs = (
        P(None, "section", "dp", "head"),
        P(None, "section", "dp", None),
        P(None, "section", "dp", "head"),
        P(None, "section", "dp"),
        P(None, "section", None, "head"),
    )
    out_specs = (
        P(None, "section", "dp", "head"),
        P(None, "section", ("dp", "head"), None),
        P("section", "dp", "head"),
    )
    body = functools.partial(relay, mesh)
    return jax.shard_map(body, mesh=mesh, in_specs=in_specs, out_specs=out_specs, check_vma=False)
```

```python
import functools

import jax
import jax.numpy as jnp
from jax import lax
from jax.experimental import pallas as pl
from jax.experimental.pallas import tpu as pltpu
from jax.sharding import PartitionSpec as P

ROPE = 64
NOPE = 128
VDIM = 128
QDIM = NOPE + ROPE
KVDIM = NOPE + VDIM
GROUP = 4
FWD, REV = 0, 1
MESH = pl.DeviceIdType.MESH


def dot(a, b, contract):
    return lax.dot_general(a, b, ((contract[:1], contract[1:]), ((), ())), preferred_element_type=jnp.float32)


def relay_kernel(
    sizes,
    queries, latents_t, out_grad, segments, weight,
    query_grad, latent_grad, weight_grad,
    q_buf, lt_buf, o_buf, w_buf, lat, rope, kv_rev, kv_all, lt_all, q_out, relay_buf, zeros, small_zeros,
    local, pieces, sums, rope_sum, w_out, seg_buf,
    q_in, lt_in, o_in, w_in, w_put, z_put, seg_in,
    kr_send, kr_recv, kf_send, kf_recv, kx_send, kx_recv, lr_send, lr_recv, lf_send, lf_recv,
    qs_send, qs_recv, rl_send, rl_recv, rf_send, hp_send, hp_recv, ls_send, ls_recv,
):
    n_section, n_dp, n_head, heads, groups = sizes
    me, my_dp, my_head = lax.axis_index("section"), lax.axis_index("dp"), lax.axis_index("head")
    mirror = n_section - 1 - me
    tokens = queries.shape[2]
    latent = weight.shape[2]
    rows = latent // n_dp
    mine = tokens // n_head
    kw, qw, ow = heads * KVDIM, heads * QDIM, heads * VDIM
    half = q_out.shape[2] // 2
    relayed = n_section == 4
    scale = QDIM ** (-0.5)

    def remote(src, dst, send, recv, **where):
        return pltpu.make_async_remote_copy(
            src_ref=src, dst_ref=dst, send_sem=send, recv_sem=recv, device_id=where, device_id_type=MESH
        )

    def dp_peer(k):
        return lax.rem(my_dp + k, n_dp)

    def dp_from(k):
        return lax.rem(my_dp + n_dp - k, n_dp)

    def head_peer(k):
        return lax.rem(my_head + k, n_head)

    def load_weight(r, g):
        cols = pl.ds(pl.multiple_of(g * kw, 128), kw)
        return pltpu.make_async_copy(weight.at[r, 0, :, cols], w_buf.at[r, g], w_in.at[r, g])

    def load_latents(r):
        return pltpu.make_async_copy(latents_t.at[r, 0], lt_buf.at[r], lt_in.at[r])

    def load_queries(r):
        return pltpu.make_async_copy(queries.at[r, 0], q_buf.at[r], q_in.at[r])

    def load_out(r):
        return pltpu.make_async_copy(out_grad.at[r, 0], o_buf.at[r], o_in.at[r])

    barrier = pltpu.get_barrier_semaphore()
    for k in range(1, n_section):
        pl.semaphore_signal(barrier, 1, device_id={"section": lax.rem(me + k, n_section)}, device_id_type=MESH)
    for k in range(1, n_dp):
        pl.semaphore_signal(barrier, 1, device_id={"dp": dp_peer(k)}, device_id_type=MESH)
        pl.semaphore_signal(barrier, 1, device_id={"section": mirror, "dp": dp_peer(k)}, device_id_type=MESH)
    for k in range(1, n_head):
        pl.semaphore_signal(barrier, 1, device_id={"head": head_peer(k)}, device_id_type=MESH)

    load_segments = pltpu.make_async_copy(segments, seg_buf, seg_in)
    load_segments.start()
    for r in (REV, FWD):
        load_latents(r).start()
        load_weight(r, 0).start()
        load_queries(r).start()
        load_out(r).start()

        @pl.loop(1, groups)
        def _(g):
            load_weight(r, g).start()

    load_segments.wait()
    zeros[...] = jnp.zeros_like(zeros)
    small_zeros[...] = jnp.zeros_like(small_zeros)
    for r in (REV, FWD):
        load_latents(r).wait()
        plain = lt_buf[r, :latent, :].astype(jnp.float32)
        lat[r] = jnp.transpose(plain).astype(jnp.bfloat16)
        rope[r] = jnp.transpose(lt_buf[r, latent:, :].astype(jnp.float32)).astype(jnp.bfloat16)
    rope_sum[...] = jnp.zeros_like(rope_sum)

    pl.semaphore_wait(barrier, n_section - 1 + 2 * (n_dp - 1) + n_head - 1)

    def latent_rev(k):
        to = dp_peer(k)
        block = pl.ds(pl.multiple_of(to * rows, rows), rows)
        return remote(
            lt_buf.at[REV, block], lt_all.at[n_dp + my_dp], lr_send.at[k], lr_recv.at[k], section=mirror, dp=to
        )

    def latent_fwd(k):
        to = dp_peer(k)
        block = pl.ds(pl.multiple_of(to * rows, rows), rows)
        return remote(lt_buf.at[FWD, block], lt_all.at[my_dp], lf_send.at[k], lf_recv.at[k], dp=to)

    for k in range(n_dp):
        latent_rev(k).start()
    for k in range(1, n_dp):
        latent_fwd(k).start()
    lt_all[my_dp] = lt_buf[FWD, pl.ds(pl.multiple_of(my_dp * rows, rows), rows), :]

    def fill(r):
        quarter = zeros.shape[1]
        return [
            pltpu.make_async_copy(zeros, query_grad.at[r, 0, :, pl.ds(c * quarter, quarter)], z_put.at[c])
            for c in range(q_out.shape[2] // quarter)
        ] + [pltpu.make_async_copy(small_zeros, latent_grad.at[r, 0], z_put.at[q_out.shape[2] // quarter])]

    def slot(piece):
        return pl.ds(pl.multiple_of(piece * tokens, tokens), tokens)

    def kv_to_mirror(g):
        return remote(kv_rev.at[g], kv_all.at[g, slot(n_dp + my_dp)], kr_send.at[g], kr_recv.at[g], section=mirror)

    def kv_to_peer(g, k):
        ref = kv_all.at[g, slot(my_dp)]
        return remote(ref, ref, kf_send.at[g, k], kf_recv.at[g, k], dp=dp_peer(k))

    def kv_passed_on(g, k):
        ref = kv_all.at[g, slot(n_dp + my_dp)]
        return remote(ref, ref, kx_send.at[g, k], kx_recv.at[g, k], dp=dp_peer(k))

    def compute(r, g, allowed):
        load_weight(r, g).wait()
        kv = dot(lat[r], w_buf[r, g], (1, 0)).astype(jnp.bfloat16)
        query_block = q_buf[r, :, pl.ds(pl.multiple_of(g * qw, 128), qw)]
        out_block = o_buf[r, :, pl.ds(pl.multiple_of(g * ow, 128), ow)]
        key_rope = rope[r]
        query_parts, kv_parts = [], []
        total = rope_sum[r]
        for h in range(heads):
            key = jnp.concatenate([kv[:, h * KVDIM : h * KVDIM + NOPE], key_rope], 1)
            value = kv[:, h * KVDIM + NOPE : (h + 1) * KVDIM]
            query = query_block[:, h * QDIM : (h + 1) * QDIM]
            out = out_block[:, h * VDIM : (h + 1) * VDIM]
            scores = jnp.where(allowed, dot(key, query, (1, 1)) * scale, jnp.float32(-1e30))
            powers = jnp.exp(scores - jnp.max(scores, axis=0, keepdims=True))
            probs = powers * (1.0 / jnp.sum(powers, axis=0, keepdims=True))
            grad_probs = dot(value, out, (1, 1))
            delta = jnp.sum(probs * grad_probs, axis=0, keepdims=True)
            score_grad = (probs * (grad_probs - delta) * scale).astype(jnp.bfloat16)
            value_grad = dot(probs.astype(jnp.bfloat16), out, (1, 0))
            key_grad = dot(score_grad, query, (1, 0))
            total += key_grad[:, NOPE:]
            query_parts.append(dot(score_grad, key, (0, 0)))
            kv_parts += [key_grad[:, :NOPE].astype(jnp.bfloat16), value_grad.astype(jnp.bfloat16)]
        rope_sum[r] = total
        q_out[r, :, pl.ds(pl.multiple_of(g * qw, 128), qw)] = jnp.concatenate(query_parts, 1).astype(jnp.bfloat16)
        kv_out = jnp.concatenate(kv_parts, 1)
        if r == REV:
            kv_rev[g] = kv_out
            kv_to_mirror(g).start()
        else:
            kv_all[g, slot(my_dp), :] = kv_out
            for k in range(1, n_dp):
                kv_to_peer(g, k).start()

    def cut(c):
        return pl.ds(c * half, half)

    def query_copy(r, c):
        to = me - 1 if r == FWD else me + 1
        return remote(
            q_out.at[r, :, cut(c)], query_grad.at[r, 0, :, cut(c)], qs_send.at[r, c], qs_recv.at[r, c], section=to
        )

    def to_relay(r):
        return remote(q_out.at[r, :, cut(0)], relay_buf, rl_send.at[r], rl_recv, section=me - 2 if r == FWD else me + 2)

    def from_relay(r):
        to = me + 1 if r == FWD else me - 1
        return remote(relay_buf, query_grad.at[r, 0, :, cut(0)], rf_send, qs_recv.at[r, 0], section=to)

    sends = {FWD: me > 0, REV: me < n_section - 1}
    receives = {FWD: me < n_section - 1, REV: me > 0}
    relays_out = {FWD: me == 2, REV: me == 1}
    relays_for = {FWD: me == 0, REV: me == 3}

    def send_queries(r):
        if relayed:

            @pl.when(relays_out[r])
            def _():
                to_relay(r).start()

            @pl.when(sends[r] & jnp.logical_not(relays_out[r]))
            def _():
                query_copy(r, 0).start()
        else:

            @pl.when(sends[r])
            def _():
                query_copy(r, 0).start()

        @pl.when(sends[r])
        def _():
            query_copy(r, 1).start()

    def head_copy(r, k):
        to = head_peer(k)
        return remote(
            local.at[r, pl.ds(pl.multiple_of(to * mine, mine), mine)],
            pieces.at[r, k - 1],
            hp_send.at[r, k],
            hp_recv.at[r, k],
            head=to,
        )

    def latent_out(r):
        to = me - 1 if r == FWD else me + 1
        return remote(sums.at[r], latent_grad.at[r, 0], ls_send.at[r], ls_recv.at[r], section=to)

    for r in (REV, FWD):
        load_queries(r).wait()
        load_out(r).wait()
        seg = jnp.broadcast_to(seg_buf[r], (tokens, tokens))
        keys = lax.broadcasted_iota(jnp.int32, (tokens, tokens), 0)
        at = lax.broadcasted_iota(jnp.int32, (tokens, tokens), 1)
        allowed = (at >= keys) & (seg == jnp.transpose(seg))

        @pl.loop(0, groups)
        def _(g):
            compute(r, g, allowed)

        send_queries(r)

    if relayed:
        for r in (REV, FWD):

            @pl.when(relays_for[r])
            def _():
                to_relay(r).wait_recv()
                from_relay(r).start()

    for r in (REV, FWD):

        def add(g, total):
            block = kv_rev[g] if r == REV else kv_all[g, slot(my_dp), :]
            return total + dot(block, w_buf[r, g], (1, 1))

        total = lax.fori_loop(0, groups, add, jnp.zeros((tokens, latent), jnp.float32))
        local[r] = jnp.concatenate([total, rope_sum[r]], 1).astype(jnp.bfloat16)
        for k in range(1, n_head):
            head_copy(r, k).start()

    for r in (REV, FWD):
        total = local[r, pl.ds(pl.multiple_of(my_head * mine, mine), mine), :].astype(jnp.float32)
        for k in range(1, n_head):
            head_copy(r, k).wait_recv()
            total += pieces[r, k - 1].astype(jnp.float32)
        sums[r] = total.astype(jnp.bfloat16)

        @pl.when(sends[r])
        def _():
            latent_out(r).start()

    for r in (FWD, REV):

        @pl.when(jnp.logical_not(receives[r]))
        def _():
            for copy in fill(r):
                copy.start()

    @pl.loop(0, groups)
    def _(g):
        kv_to_mirror(g).wait_recv()
        for k in range(1, n_dp):
            kv_passed_on(g, k).start()

    for k in range(n_dp):
        latent_rev(k).wait_recv()
    for k in range(1, n_dp):
        latent_fwd(k).wait_recv()
    latent_rows = jnp.concatenate([lt_all[p] for p in range(2 * n_dp)], 1)

    def put_weight(g):
        return pltpu.make_async_copy(
            w_out.at[g], weight_grad.at[0, :, pl.ds(pl.multiple_of(g * kw, 128), kw)], w_put.at[g]
        )

    @pl.loop(0, groups)
    def _(g):
        for k in range(1, n_dp):
            kv_to_peer(g, k).wait_recv()
            kv_passed_on(g, k).wait_recv()
        w_out[g] = dot(latent_rows, kv_all[g], (1, 0))
        put_weight(g).start()

    @pl.loop(0, groups)
    def _(g):
        put_weight(g).wait()
        kv_to_mirror(g).wait_send()
        for k in range(1, n_dp):
            kv_to_peer(g, k).wait_send()
            kv_passed_on(g, k).wait_send()

    for k in range(n_dp):
        latent_rev(k).wait_send()
    for k in range(1, n_dp):
        latent_fwd(k).wait_send()
    for r in (REV, FWD):
        for k in range(1, n_head):
            head_copy(r, k).wait_send()

        @pl.when(jnp.logical_not(receives[r]))
        def _():
            for copy in fill(r):
                copy.wait()

        if relayed:

            @pl.when(relays_out[r])
            def _():
                to_relay(r).wait_send()

            @pl.when(sends[r] & jnp.logical_not(relays_out[r]))
            def _():
                query_copy(r, 0).wait_send()

            @pl.when(relays_for[r])
            def _():
                from_relay(r).wait_send()
        else:

            @pl.when(sends[r])
            def _():
                query_copy(r, 0).wait_send()

        @pl.when(sends[r])
        def _():
            query_copy(r, 1).wait_send()
            latent_out(r).wait_send()

        @pl.when(receives[r])
        def _():
            query_copy(r, 0).wait_recv()
            query_copy(r, 1).wait_recv()
            latent_out(r).wait_recv()


def relay(mesh, queries, latents, out_grad, segment_ids, up_weight):
    n_section, n_dp, n_head = (mesh.shape[a] for a in ("section", "dp", "head"))
    tokens = queries.shape[2]
    latent, width = up_weight.shape[2:]
    features = latents.shape[3]
    heads_here = width // KVDIM
    heads = next(k for k in (GROUP, 2, heads_here) if heads_here % k == 0)
    groups = heads_here // heads
    rows, mine = latent // n_dp, tokens // n_head
    kw = heads * KVDIM
    q_width = heads_here * QDIM
    quarter = q_width // 4
    dma = pltpu.SemaphoreType.DMA
    bf16, f32 = jnp.bfloat16, jnp.float32
    anywhere = pl.BlockSpec(memory_space=pl.ANY)
    args = (queries, jnp.swapaxes(latents, 2, 3), out_grad, segment_ids, up_weight)
    flops = 2 * (2 * tokens * width * latent * 2 + 2 * tokens * tokens * heads_here * 5 * KVDIM)
    return pl.pallas_call(
        functools.partial(relay_kernel, (n_section, n_dp, n_head, heads, groups)),
        in_specs=[anywhere] * 5,
        out_specs=[anywhere] * 3,
        out_shape=[
            jax.ShapeDtypeStruct((2, 1, tokens, q_width), bf16),
            jax.ShapeDtypeStruct((2, 1, mine, features), bf16),
            jax.ShapeDtypeStruct((1, rows, width), f32),
        ],
        scratch_shapes=[
            pltpu.VMEM((2, tokens, q_width), bf16),
            pltpu.VMEM((2, features, tokens), bf16),
            pltpu.VMEM((2, tokens, heads_here * VDIM), bf16),
            pltpu.VMEM((2, groups, latent, kw), bf16),
            pltpu.VMEM((2, tokens, latent), bf16),
            pltpu.VMEM((2, tokens, features - latent), bf16),
            pltpu.VMEM((groups, tokens, kw), bf16),
            pltpu.VMEM((groups, 2 * n_dp * tokens, kw), bf16),
            pltpu.VMEM((2 * n_dp, rows, tokens), bf16),
            pltpu.VMEM((2, tokens, q_width), bf16),
            pltpu.VMEM((tokens, q_width // 2), bf16),
            pltpu.VMEM((tokens, quarter), bf16),
            pltpu.VMEM((mine, features), bf16),
            pltpu.VMEM((2, tokens, features), bf16),
            pltpu.VMEM((2, n_head - 1, mine, features), bf16),
            pltpu.VMEM((2, mine, features), bf16),
            pltpu.VMEM((2, tokens, features - latent), f32),
            pltpu.VMEM((groups, rows, kw), f32),
            pltpu.VMEM((2, 1, tokens), jnp.int32),
            dma((2,)), dma((2,)), dma((2,)), dma((2, groups)), dma((groups,)), dma((5,)), dma,
            dma((groups,)), dma((groups,)), dma((groups, n_dp)), dma((groups, n_dp)),
            dma((groups, n_dp)), dma((groups, n_dp)), dma((n_dp,)), dma((n_dp,)), dma((n_dp,)), dma((n_dp,)),
            dma((2, 2)), dma((2, 2)), dma((2,)), dma, dma, dma((2, n_head)), dma((2, n_head)), dma((2,)), dma((2,)),
        ],
        compiler_params=pltpu.CompilerParams(collective_id=0, has_side_effects=True, vmem_limit_bytes=44 << 20),
        cost_estimate=pl.CostEstimate(flops=flops, bytes_accessed=8 * latent * width, transcendentals=0),
        name="relay",
    )(*(pltpu.with_memory_space_constraint(x, pltpu.HBM) for x in args))


def unload_kernel(count, *refs):
    copies = [pltpu.make_async_copy(refs[k], refs[count + k], refs[-1].at[k]) for k in range(count)]
    for copy in copies:
        copy.start()
    for copy in copies:
        copy.wait()


def unload(*arrays):
    count = len(arrays)
    return pl.pallas_call(
        functools.partial(unload_kernel, count),
        in_specs=[pl.BlockSpec(memory_space=pl.ANY)] * count,
        out_specs=[pl.BlockSpec(memory_space=pl.ANY)] * count,
        out_shape=[pltpu.HBM(x.shape, x.dtype) for x in arrays],
        scratch_shapes=[pltpu.SemaphoreType.DMA((count,))],
        compiler_params=pltpu.CompilerParams(vmem_limit_bytes=1 << 20),
        name="unload",
    )(*arrays)


def solution(mesh):
    in_specs = (
        P(None, "section", "dp", "head"),
        P(None, "section", "dp", None),
        P(None, "section", "dp", "head"),
        P(None, "section", "dp"),
        P(None, "section", None, "head"),
    )
    out_specs = (
        P(None, "section", "dp", "head"),
        P(None, "section", ("dp", "head"), None),
        P("section", "dp", "head"),
    )
    def body(*args):
        return unload(*relay(mesh, *args))

    return jax.shard_map(body, mesh=mesh, in_specs=in_specs, out_specs=out_specs, check_vma=False)
```

```python
import functools

import jax
import jax.numpy as jnp
from jax import lax
from jax.experimental import pallas as pl
from jax.experimental.pallas import tpu as pltpu
from jax.sharding import PartitionSpec as P

ROPE = 64
NOPE = 128
VDIM = 128
QDIM = NOPE + ROPE
KVDIM = NOPE + VDIM
GROUP = 4
FWD, REV = 0, 1
MESH = pl.DeviceIdType.MESH


def dot(a, b, contract):
    return lax.dot_general(a, b, ((contract[:1], contract[1:]), ((), ())), preferred_element_type=jnp.float32)


def relay_kernel(
    sizes,
    queries, latents_t, out_grad, segments, weight,
    query_grad, latent_grad, weight_grad,
    q_buf, lt_buf, o_buf, w_buf, lat, rope, kv_rev, kv_all, lt_all, q_out, relay_buf, zeros, small_zeros,
    local, pieces, sums, rope_sum, w_out, seg_buf,
    q_in, lt_in, o_in, w_in, w_put, z_put, seg_in,
    kr_send, kr_recv, kf_send, kf_recv, kx_send, kx_recv, lr_send, lr_recv, lf_send, lf_recv, lx_send, lx_recv,
    qs_send, qs_recv, rl_send, rl_recv, rf_send, hp_send, hp_recv, ls_send, ls_recv,
):
    n_section, n_dp, n_head, heads, groups = sizes
    me, my_dp, my_head = lax.axis_index("section"), lax.axis_index("dp"), lax.axis_index("head")
    mirror = n_section - 1 - me
    tokens = queries.shape[2]
    latent = weight.shape[2]
    rows = latent // n_dp
    mine = tokens // n_head
    parts = min(n_head, rows // 16)
    part = rows // parts
    kw, qw, ow = heads * KVDIM, heads * QDIM, heads * VDIM
    half = q_out.shape[2] // 2
    relayed = n_section == 4
    scale = QDIM ** (-0.5)

    def remote(src, dst, send, recv, **where):
        return pltpu.make_async_remote_copy(
            src_ref=src, dst_ref=dst, send_sem=send, recv_sem=recv, device_id=where, device_id_type=MESH
        )

    def dp_peer(k):
        return lax.rem(my_dp + k, n_dp)

    def head_peer(k):
        return lax.rem(my_head + k, n_head)

    def load_weight(r, g):
        cols = pl.ds(pl.multiple_of(g * kw, 128), kw)
        return pltpu.make_async_copy(weight.at[r, 0, :, cols], w_buf.at[r, g], w_in.at[r, g])

    def load_latents(r):
        return pltpu.make_async_copy(latents_t.at[r, 0], lt_buf.at[r], lt_in.at[r])

    def load_queries(r, g):
        cols = pl.ds(pl.multiple_of(g * qw, 128), qw)
        return pltpu.make_async_copy(queries.at[r, 0, :, cols], q_buf.at[r, g], q_in.at[r, g])

    def load_out(r, g):
        cols = pl.ds(pl.multiple_of(g * ow, 128), ow)
        return pltpu.make_async_copy(out_grad.at[r, 0, :, cols], o_buf.at[r, g], o_in.at[r, g])

    def start_loads(r, g):
        load_weight(r, g).start()
        load_queries(r, g).start()
        load_out(r, g).start()

    def wait_loads(r, g):
        load_weight(r, g).wait()
        load_queries(r, g).wait()
        load_out(r, g).wait()

    barrier = pltpu.get_barrier_semaphore()
    for k in range(1, n_section):
        pl.semaphore_signal(barrier, 1, device_id={"section": lax.rem(me + k, n_section)}, device_id_type=MESH)
    for k in range(1, n_dp):
        pl.semaphore_signal(barrier, 1, device_id={"dp": dp_peer(k)}, device_id_type=MESH)
        pl.semaphore_signal(barrier, 1, device_id={"section": mirror, "dp": dp_peer(k)}, device_id_type=MESH)
    for k in range(1, n_head):
        pl.semaphore_signal(barrier, 1, device_id={"head": head_peer(k)}, device_id_type=MESH)

    load_segments = pltpu.make_async_copy(segments, seg_buf, seg_in)
    load_latents(REV).start()
    start_loads(REV, 0)
    load_segments.start()

    def latents_in(r):
        lat[r] = jnp.transpose(lt_buf[r, :latent, :].astype(jnp.float32)).astype(jnp.bfloat16)
        rope[r] = jnp.transpose(lt_buf[r, latent:, :].astype(jnp.float32)).astype(jnp.bfloat16)

    load_latents(REV).wait()
    pl.semaphore_wait(barrier, n_section - 1 + 2 * (n_dp - 1) + n_head - 1)

    def latent_rev(k):
        to = dp_peer(k)
        block = pl.ds(pl.multiple_of(to * rows + my_head * part, part), part)
        return remote(
            lt_buf.at[REV, block],
            lt_all.at[n_dp + my_dp, pl.ds(pl.multiple_of(my_head * part, part), part)],
            lr_send.at[k],
            lr_recv.at[k],
            section=mirror,
            dp=to,
        )

    def latent_fwd(k):
        to = dp_peer(k)
        block = pl.ds(pl.multiple_of(to * rows, rows), rows)
        return remote(lt_buf.at[FWD, block], lt_all.at[my_dp], lf_send.at[k], lf_recv.at[k], dp=to)

    def latent_parts(d, k):
        ref = lt_all.at[n_dp + d, pl.ds(pl.multiple_of(my_head * part, part), part)]
        return remote(ref, ref, lx_send.at[d, k], lx_recv.at[d, k], head=head_peer(k))

    def holds_part(head, do):
        if parts == n_head:
            do()
        else:
            pl.when(head < parts)(do)

    @functools.partial(holds_part, my_head)
    def _():
        for k in range(n_dp):
            latent_rev(k).start()

    def fill(r):
        quarter = zeros.shape[1]
        return [
            pltpu.make_async_copy(zeros, query_grad.at[r, 0, :, pl.ds(c * quarter, quarter)], z_put.at[c])
            for c in range(q_out.shape[2] // quarter)
        ] + [pltpu.make_async_copy(small_zeros, latent_grad.at[r, 0], z_put.at[q_out.shape[2] // quarter])]

    def slot(piece):
        return pl.ds(pl.multiple_of(piece * tokens, tokens), tokens)

    def kv_to_mirror(g):
        return remote(kv_rev.at[g], kv_all.at[g, slot(n_dp + my_dp)], kr_send.at[g], kr_recv.at[g], section=mirror)

    def kv_to_peer(g, k):
        ref = kv_all.at[g, slot(my_dp)]
        return remote(ref, ref, kf_send.at[g, k], kf_recv.at[g, k], dp=dp_peer(k))

    def kv_passed_on(g, k):
        ref = kv_all.at[g, slot(n_dp + my_dp)]
        return remote(ref, ref, kx_send.at[g, k], kx_recv.at[g, k], dp=dp_peer(k))

    def compute(r, g, allowed):
        pl.when(g > 0)(lambda: wait_loads(r, g))
        kv = dot(lat[r], w_buf[r, g], (1, 0)).astype(jnp.bfloat16)
        query_block = q_buf[r, g]
        out_block = o_buf[r, g]
        key_rope = rope[r]
        query_parts, kv_parts = [], []
        total = rope_sum[r]
        for h in range(heads):
            key = jnp.concatenate([kv[:, h * KVDIM : h * KVDIM + NOPE], key_rope], 1)
            value = kv[:, h * KVDIM + NOPE : (h + 1) * KVDIM]
            query = query_block[:, h * QDIM : (h + 1) * QDIM]
            out = out_block[:, h * VDIM : (h + 1) * VDIM]
            scores = jnp.where(allowed, dot(key, query, (1, 1)) * scale, jnp.float32(-1e30))
            powers = jnp.exp(scores - jnp.max(scores, axis=0, keepdims=True))
            probs = powers * (1.0 / jnp.sum(powers, axis=0, keepdims=True))
            grad_probs = dot(value, out, (1, 1))
            delta = jnp.sum(probs * grad_probs, axis=0, keepdims=True)
            score_grad = (probs * (grad_probs - delta) * scale).astype(jnp.bfloat16)
            value_grad = dot(probs.astype(jnp.bfloat16), out, (1, 0))
            key_grad = dot(score_grad, query, (1, 0))
            total += key_grad[:, NOPE:]
            query_parts.append(dot(score_grad, key, (0, 0)))
            kv_parts += [key_grad[:, :NOPE].astype(jnp.bfloat16), value_grad.astype(jnp.bfloat16)]
        rope_sum[r] = total
        q_out[r, :, pl.ds(pl.multiple_of(g * qw, 128), qw)] = jnp.concatenate(query_parts, 1).astype(jnp.bfloat16)
        kv_out = jnp.concatenate(kv_parts, 1)
        if r == REV:
            kv_rev[g] = kv_out
            kv_to_mirror(g).start()
        else:
            kv_all[g, slot(my_dp), :] = kv_out
            for k in range(1, n_dp):
                kv_to_peer(g, k).start()

    def cut(c):
        return pl.ds(c * half, half)

    def query_copy(r, c):
        to = me - 1 if r == FWD else me + 1
        return remote(
            q_out.at[r, :, cut(c)], query_grad.at[r, 0, :, cut(c)], qs_send.at[r, c], qs_recv.at[r, c], section=to
        )

    def to_relay(r):
        return remote(q_out.at[r, :, cut(0)], relay_buf, rl_send.at[r], rl_recv, section=me - 2 if r == FWD else me + 2)

    def from_relay(r):
        to = me + 1 if r == FWD else me - 1
        return remote(relay_buf, query_grad.at[r, 0, :, cut(0)], rf_send, qs_recv.at[r, 0], section=to)

    sends = {FWD: me > 0, REV: me < n_section - 1}
    receives = {FWD: me < n_section - 1, REV: me > 0}
    relays_out = {FWD: me == 2, REV: me == 1}
    relays_for = {FWD: me == 0, REV: me == 3}

    def send_queries(r):
        @pl.when(sends[r] & jnp.logical_not(relays_out[r]) if relayed else sends[r])
        def _():
            query_copy(r, 0).start()

        @pl.when(sends[r])
        def _():
            query_copy(r, 1).start()

    def head_copy(r, k):
        to = head_peer(k)
        return remote(
            local.at[r, pl.ds(pl.multiple_of(to * mine, mine), mine)],
            pieces.at[r, k - 1],
            hp_send.at[r, k],
            hp_recv.at[r, k],
            head=to,
        )

    def latent_out(r):
        to = me - 1 if r == FWD else me + 1
        return remote(sums.at[r], latent_grad.at[r, 0], ls_send.at[r], ls_recv.at[r], section=to)

    keys = lax.broadcasted_iota(jnp.int32, (tokens, tokens), 0)
    at = lax.broadcasted_iota(jnp.int32, (tokens, tokens), 1)

    def run(r):
        latents_in(r)
        seg = jnp.broadcast_to(seg_buf[r], (tokens, tokens))
        allowed = (at >= keys) & (seg == jnp.transpose(seg))

        @pl.loop(0, groups)
        def _(g):
            compute(r, g, allowed)

        if relayed:

            @pl.when(relays_out[r])
            def _():
                to_relay(r).start()

    load_segments.wait()
    rope_sum[...] = jnp.zeros_like(rope_sum)
    wait_loads(REV, 0)

    @pl.loop(1, groups)
    def _(g):
        start_loads(REV, g)

    load_latents(FWD).start()

    @pl.loop(0, groups)
    def _(g):
        start_loads(FWD, g)

    run(REV)
    load_latents(FWD).wait()
    for k in range(1, n_dp):
        latent_fwd(k).start()
    lt_all[my_dp] = lt_buf[FWD, pl.ds(pl.multiple_of(my_dp * rows, rows), rows), :]
    wait_loads(FWD, 0)
    run(FWD)

    for r in (REV, FWD):

        def add(g, total):
            block = kv_rev[g] if r == REV else kv_all[g, slot(my_dp), :]
            return total + dot(block, w_buf[r, g], (1, 1))

        total = lax.fori_loop(0, groups, add, jnp.zeros((tokens, latent), jnp.float32))
        local[r] = jnp.concatenate([total, rope_sum[r]], 1).astype(jnp.bfloat16)
        for k in range(1, n_head):
            head_copy(r, k).start()

    for r in (REV, FWD):
        total = local[r, pl.ds(pl.multiple_of(my_head * mine, mine), mine), :].astype(jnp.float32)
        for k in range(1, n_head):
            head_copy(r, k).wait_recv()
            total += pieces[r, k - 1].astype(jnp.float32)
        sums[r] = total.astype(jnp.bfloat16)

        @pl.when(sends[r])
        def _():
            latent_out(r).start()

    @pl.when(me < n_section // 2)
    def _():
        send_queries(REV)
        send_queries(FWD)

    @pl.when(me >= n_section // 2)
    def _():
        send_queries(FWD)
        send_queries(REV)

    zeros[...] = jnp.zeros_like(zeros)
    small_zeros[...] = jnp.zeros_like(small_zeros)
    for r in (FWD, REV):

        @pl.when(jnp.logical_not(receives[r]))
        def _():
            for copy in fill(r):
                copy.start()

    @functools.partial(holds_part, my_head)
    def _():
        for k in range(n_dp):
            latent_rev(k).wait_recv()
        for d in range(n_dp):
            for k in range(1, n_head):
                latent_parts(d, k).start()

    @pl.loop(0, groups)
    def _(g):
        kv_to_mirror(g).wait_recv()
        for k in range(1, n_dp):
            kv_passed_on(g, k).start()

    if relayed:
        for r in (REV, FWD):

            @pl.when(relays_for[r])
            def _():
                to_relay(r).wait_recv()
                from_relay(r).start()

    for k in range(1, n_head):

        @functools.partial(holds_part, lax.rem(my_head + n_head - k, n_head))
        def _():
            for d in range(n_dp):
                latent_parts(d, k).wait_recv()

    for k in range(1, n_dp):
        latent_fwd(k).wait_recv()
    latent_rows = jnp.concatenate([lt_all[p] for p in range(2 * n_dp)], 1)

    def put_weight(g):
        return pltpu.make_async_copy(
            w_out.at[g], weight_grad.at[0, :, pl.ds(pl.multiple_of(g * kw, 128), kw)], w_put.at[g]
        )

    @pl.loop(0, groups)
    def _(g):
        for k in range(1, n_dp):
            kv_to_peer(g, k).wait_recv()
            kv_passed_on(g, k).wait_recv()
        w_out[g] = dot(latent_rows, kv_all[g], (1, 0))
        put_weight(g).start()

    @pl.loop(0, groups)
    def _(g):
        put_weight(g).wait()
        kv_to_mirror(g).wait_send()
        for k in range(1, n_dp):
            kv_to_peer(g, k).wait_send()
            kv_passed_on(g, k).wait_send()

    @functools.partial(holds_part, my_head)
    def _():
        for k in range(n_dp):
            latent_rev(k).wait_send()
        for d in range(n_dp):
            for k in range(1, n_head):
                latent_parts(d, k).wait_send()

    for k in range(1, n_dp):
        latent_fwd(k).wait_send()
    for r in (REV, FWD):
        for k in range(1, n_head):
            head_copy(r, k).wait_send()

        @pl.when(jnp.logical_not(receives[r]))
        def _():
            for copy in fill(r):
                copy.wait()

        if relayed:

            @pl.when(relays_out[r])
            def _():
                to_relay(r).wait_send()

            @pl.when(sends[r] & jnp.logical_not(relays_out[r]))
            def _():
                query_copy(r, 0).wait_send()

            @pl.when(relays_for[r])
            def _():
                from_relay(r).wait_send()
        else:

            @pl.when(sends[r])
            def _():
                query_copy(r, 0).wait_send()

        @pl.when(sends[r])
        def _():
            query_copy(r, 1).wait_send()
            latent_out(r).wait_send()

        @pl.when(receives[r])
        def _():
            query_copy(r, 0).wait_recv()
            query_copy(r, 1).wait_recv()
            latent_out(r).wait_recv()


def relay(mesh, queries, latents, out_grad, segment_ids, up_weight):
    n_section, n_dp, n_head = (mesh.shape[a] for a in ("section", "dp", "head"))
    tokens = queries.shape[2]
    latent, width = up_weight.shape[2:]
    features = latents.shape[3]
    heads_here = width // KVDIM
    heads = next(k for k in (GROUP, 2, heads_here) if heads_here % k == 0)
    groups = heads_here // heads
    rows, mine = latent // n_dp, tokens // n_head
    kw = heads * KVDIM
    q_width = heads_here * QDIM
    quarter = q_width // 4
    dma = pltpu.SemaphoreType.DMA
    bf16, f32 = jnp.bfloat16, jnp.float32
    anywhere = pl.BlockSpec(memory_space=pl.ANY)
    args = (queries, jnp.swapaxes(latents, 2, 3), out_grad, segment_ids, up_weight)
    flops = 2 * (2 * tokens * width * latent * 2 + 2 * tokens * tokens * heads_here * 5 * KVDIM)
    return pl.pallas_call(
        functools.partial(relay_kernel, (n_section, n_dp, n_head, heads, groups)),
        in_specs=[anywhere] * 5,
        out_specs=[anywhere] * 3,
        out_shape=[
            jax.ShapeDtypeStruct((2, 1, tokens, q_width), bf16),
            jax.ShapeDtypeStruct((2, 1, mine, features), bf16),
            jax.ShapeDtypeStruct((1, rows, width), f32),
        ],
        scratch_shapes=[
            pltpu.VMEM((2, groups, tokens, heads * QDIM), bf16),
            pltpu.VMEM((2, features, tokens), bf16),
            pltpu.VMEM((2, groups, tokens, heads * VDIM), bf16),
            pltpu.VMEM((2, groups, latent, kw), bf16),
            pltpu.VMEM((2, tokens, latent), bf16),
            pltpu.VMEM((2, tokens, features - latent), bf16),
            pltpu.VMEM((groups, tokens, kw), bf16),
            pltpu.VMEM((groups, 2 * n_dp * tokens, kw), bf16),
            pltpu.VMEM((2 * n_dp, rows, tokens), bf16),
            pltpu.VMEM((2, tokens, q_width), bf16),
            pltpu.VMEM((tokens, q_width // 2), bf16),
            pltpu.VMEM((tokens, quarter), bf16),
            pltpu.VMEM((mine, features), bf16),
            pltpu.VMEM((2, tokens, features), bf16),
            pltpu.VMEM((2, n_head - 1, mine, features), bf16),
            pltpu.VMEM((2, mine, features), bf16),
            pltpu.VMEM((2, tokens, features - latent), f32),
            pltpu.VMEM((groups, rows, kw), f32),
            pltpu.VMEM((2, 1, tokens), jnp.int32),
            dma((2, groups)), dma((2,)), dma((2, groups)), dma((2, groups)), dma((groups,)), dma((5,)), dma,
            dma((groups,)), dma((groups,)), dma((groups, n_dp)), dma((groups, n_dp)),
            dma((groups, n_dp)), dma((groups, n_dp)), dma((n_dp,)), dma((n_dp,)), dma((n_dp,)), dma((n_dp,)),
            dma((n_dp, n_head)), dma((n_dp, n_head)),
            dma((2, 2)), dma((2, 2)), dma((2,)), dma, dma, dma((2, n_head)), dma((2, n_head)), dma((2,)), dma((2,)),
        ],
        compiler_params=pltpu.CompilerParams(collective_id=0, has_side_effects=True, vmem_limit_bytes=44 << 20),
        cost_estimate=pl.CostEstimate(flops=flops, bytes_accessed=8 * latent * width, transcendentals=0),
        name="relay",
    )(*(pltpu.with_memory_space_constraint(x, pltpu.HBM) for x in args))


def unload_kernel(count, *refs):
    copies = [pltpu.make_async_copy(refs[k], refs[count + k], refs[-1].at[k]) for k in range(count)]
    for copy in copies:
        copy.start()
    for copy in copies:
        copy.wait()


def unload(*arrays):
    count = len(arrays)
    return pl.pallas_call(
        functools.partial(unload_kernel, count),
        in_specs=[pl.BlockSpec(memory_space=pl.ANY)] * count,
        out_specs=[pl.BlockSpec(memory_space=pl.ANY)] * count,
        out_shape=[pltpu.HBM(x.shape, x.dtype) for x in arrays],
        scratch_shapes=[pltpu.SemaphoreType.DMA((count,))],
        compiler_params=pltpu.CompilerParams(vmem_limit_bytes=1 << 20),
        name="unload",
    )(*arrays)


def solution(mesh):
    in_specs = (
        P(None, "section", "dp", "head"),
        P(None, "section", "dp", None),
        P(None, "section", "dp", "head"),
        P(None, "section", "dp"),
        P(None, "section", None, "head"),
    )
    out_specs = (
        P(None, "section", "dp", "head"),
        P(None, "section", ("dp", "head"), None),
        P("section", "dp", "head"),
    )
    def body(*args):
        return unload(*relay(mesh, *args))

    return jax.shard_map(body, mesh=mesh, in_specs=in_specs, out_specs=out_specs, check_vma=False)
```

```python
import functools

import jax
import jax.numpy as jnp
from jax import lax
from jax.experimental import pallas as pl
from jax.experimental.pallas import tpu as pltpu
from jax.sharding import PartitionSpec as P

ROPE = 64
NOPE = 128
VDIM = 128
QDIM = NOPE + ROPE
KVDIM = NOPE + VDIM
GROUP = 4
CUTS = 4
BLOCKS = 1
RELAYED = (10, 7)
FWD, REV = 0, 1
MESH = pl.DeviceIdType.MESH


def dot(a, b, contract):
    return lax.dot_general(a, b, ((contract[:1], contract[1:]), ((), ())), preferred_element_type=jnp.float32)


def relay_kernel(
    sizes,
    queries, latents_t, out_grad, segments, weight,
    query_grad, latent_grad, weight_grad,
    q_buf, lt_buf, o_buf, w_buf, lat, rope, kv_rev, kv_all, lt_all, q_out, relay_buf, zeros, small_zeros,
    local, pieces, sums, rope_sum, w_out, seg_buf,
    q_in, lt_in, o_in, w_in, w_put, z_put, seg_in,
    kr_send, kr_recv, kf_send, kf_recv, kx_send, kx_recv, lr_send, lr_recv, lf_send, lf_recv, lx_send, lx_recv,
    qs_send, qs_recv, rl_send, rl_recv, rf_send, hp_send, hp_recv, ls_send, ls_recv,
):
    n_section, n_dp, n_head, heads, groups = sizes
    me, my_dp, my_head = lax.axis_index("section"), lax.axis_index("dp"), lax.axis_index("head")
    mirror = n_section - 1 - me
    tokens = queries.shape[2]
    latent = weight.shape[2]
    rows = latent // n_dp
    mine = tokens // n_head
    parts = min(n_head, rows // 16)
    part = rows // parts
    kw, qw, ow = heads * KVDIM, heads * QDIM, heads * VDIM
    relayed = relay_buf.shape[0] > 1
    height = tokens // CUTS
    scale = QDIM ** (-0.5)

    def remote(src, dst, send, recv, **where):
        return pltpu.make_async_remote_copy(
            src_ref=src, dst_ref=dst, send_sem=send, recv_sem=recv, device_id=where, device_id_type=MESH
        )

    def dp_peer(k):
        return lax.rem(my_dp + k, n_dp)

    def head_peer(k):
        return lax.rem(my_head + k, n_head)

    def load_weight(r, g):
        cols = pl.ds(pl.multiple_of(g * kw, 128), kw)
        return pltpu.make_async_copy(weight.at[r, 0, :, cols], w_buf.at[r, g], w_in.at[r, g])

    half = heads // 2
    early = heads % 4 == 0

    def load_early(first):
        cols = pl.ds(first * KVDIM, half * KVDIM)
        return pltpu.make_async_copy(
            weight.at[REV, 0, :, cols], w_buf.at[REV, 0, :, cols], w_in.at[REV, groups * min(first, 1)]
        )

    def load_latents(r):
        return pltpu.make_async_copy(latents_t.at[r, 0], lt_buf.at[r], lt_in.at[r])

    def load_queries(r, g):
        cols = pl.ds(pl.multiple_of(g * qw, 128), qw)
        return pltpu.make_async_copy(queries.at[r, 0, :, cols], q_buf.at[r, g], q_in.at[r, g])

    def load_out(r, g):
        cols = pl.ds(pl.multiple_of(g * ow, 128), ow)
        return pltpu.make_async_copy(out_grad.at[r, 0, :, cols], o_buf.at[r, g], o_in.at[r, g])

    def start_loads(r, g):
        load_weight(r, g).start()
        load_queries(r, g).start()
        load_out(r, g).start()

    def wait_loads(r, g):
        load_weight(r, g).wait()
        load_queries(r, g).wait()
        load_out(r, g).wait()

    barrier = pltpu.get_barrier_semaphore()
    for k in range(1, n_section):
        pl.semaphore_signal(barrier, 1, device_id={"section": lax.rem(me + k, n_section)}, device_id_type=MESH)
    for k in range(1, n_dp):
        pl.semaphore_signal(barrier, 1, device_id={"dp": dp_peer(k)}, device_id_type=MESH)
        for section in [lax.rem(me + j, n_section) for j in range(1, n_section)] if relayed else [mirror]:
            pl.semaphore_signal(barrier, 1, device_id={"section": section, "dp": dp_peer(k)}, device_id_type=MESH)
    for k in range(1, n_head):
        pl.semaphore_signal(barrier, 1, device_id={"head": head_peer(k)}, device_id_type=MESH)

    load_segments = pltpu.make_async_copy(segments, seg_buf, seg_in)
    load_latents(REV).start()
    if early:
        load_early(0).start()
        load_queries(REV, 0).start()
        load_out(REV, 0).start()
        load_early(half).start()
    else:
        start_loads(REV, 0)
    load_segments.start()

    def latents_in(r):
        lat[r] = jnp.transpose(lt_buf[r, :latent, :].astype(jnp.float32)).astype(jnp.bfloat16)
        rope[r] = jnp.transpose(lt_buf[r, latent:, :].astype(jnp.float32)).astype(jnp.bfloat16)

    load_latents(REV).wait()
    pl.semaphore_wait(barrier, n_section - 1 + (n_section if relayed else 2) * (n_dp - 1) + n_head - 1)

    def latent_rev(k):
        to = dp_peer(k)
        block = pl.ds(pl.multiple_of(to * rows + my_head * part, part), part)
        return remote(
            lt_buf.at[REV, block],
            lt_all.at[n_dp + my_dp, pl.ds(pl.multiple_of(my_head * part, part), part)],
            lr_send.at[k],
            lr_recv.at[k],
            section=mirror,
            dp=to,
        )

    def latent_fwd(k):
        to = dp_peer(k)
        block = pl.ds(pl.multiple_of(to * rows, rows), rows)
        return remote(lt_buf.at[FWD, block], lt_all.at[my_dp], lf_send.at[k], lf_recv.at[k], dp=to)

    def latent_parts(d, k):
        ref = lt_all.at[n_dp + d, pl.ds(pl.multiple_of(my_head * part, part), part)]
        return remote(ref, ref, lx_send.at[d, k], lx_recv.at[d, k], head=head_peer(k))

    def holds_part(head, do):
        if parts == n_head:
            do()
        else:
            pl.when(head < parts)(do)

    @functools.partial(holds_part, my_head)
    def _():
        for k in range(n_dp):
            latent_rev(k).start()

    def fill(r):
        return [
            pltpu.make_async_copy(zeros, query_grad.at[r, g], z_put.at[g]) for g in range(groups)
        ] + [pltpu.make_async_copy(small_zeros, latent_grad.at[r, 0], z_put.at[groups])]

    def slot(piece):
        return pl.ds(pl.multiple_of(piece * tokens, tokens), tokens)

    def kv_to_mirror(g):
        return remote(kv_rev.at[g], kv_all.at[g, slot(n_dp + my_dp)], kr_send.at[g], kr_recv.at[g], section=mirror)

    def early_to_mirror(first):
        cols, sem = pl.ds(first * KVDIM, half * KVDIM), groups * min(first, 1)
        return remote(
            kv_rev.at[0, :, cols], kv_all.at[0, slot(n_dp + my_dp), cols], kr_send.at[sem], kr_recv.at[sem], section=mirror
        )

    def kv_to_peer(g, k):
        ref = kv_all.at[g, slot(my_dp)]
        return remote(ref, ref, kf_send.at[g, k], kf_recv.at[g, k], dp=dp_peer(k))

    def kv_passed_on(g, k):
        ref = kv_all.at[g, slot(n_dp + my_dp)]
        return remote(ref, ref, kx_send.at[g, k], kx_recv.at[g, k], dp=dp_peer(k))

    def compute(r, g, allowed, first=0, end=heads):
        kv = dot(lat[r], w_buf[r, g, :, first * KVDIM : end * KVDIM], (1, 0)).astype(jnp.bfloat16)
        query_block = q_buf[r, g, :, first * QDIM : end * QDIM]
        out_block = o_buf[r, g, :, first * VDIM : end * VDIM]
        key_rope = rope[r]
        query_parts, kv_parts = [], []
        total = rope_sum[r]
        for h in range(end - first):
            key = jnp.concatenate([kv[:, h * KVDIM : h * KVDIM + NOPE], key_rope], 1)
            value = kv[:, h * KVDIM + NOPE : (h + 1) * KVDIM]
            query = query_block[:, h * QDIM : (h + 1) * QDIM]
            out = out_block[:, h * VDIM : (h + 1) * VDIM]
            scores = jnp.where(allowed, dot(key, query, (1, 1)) * scale, jnp.float32(-1e30))
            powers = jnp.exp(scores - jnp.max(scores, axis=0, keepdims=True))
            probs = powers * (1.0 / jnp.sum(powers, axis=0, keepdims=True))
            grad_probs = dot(value, out, (1, 1))
            delta = jnp.sum(probs * grad_probs, axis=0, keepdims=True)
            score_grad = (probs * (grad_probs - delta) * scale).astype(jnp.bfloat16)
            value_grad = dot(probs.astype(jnp.bfloat16), out, (1, 0))
            key_grad = dot(score_grad, query, (1, 0))
            total += key_grad[:, NOPE:]
            query_parts.append(dot(score_grad, key, (0, 0)))
            kv_parts += [key_grad[:, :NOPE].astype(jnp.bfloat16), value_grad.astype(jnp.bfloat16)]
        rope_sum[r] = total
        q_out[r, g, :, first * QDIM : end * QDIM] = jnp.concatenate(query_parts, 1).astype(jnp.bfloat16)
        kv_out = jnp.concatenate(kv_parts, 1)
        if r == REV:
            kv_rev[g, :, first * KVDIM : end * KVDIM] = kv_out
            (kv_to_mirror(g) if end - first == heads else early_to_mirror(first)).start()
        else:
            kv_all[g, slot(my_dp), :] = kv_out
            for k in range(1, n_dp):
                kv_to_peer(g, k).start()

    def piece(ref, r, p):
        return ref.at[r, p // CUTS, pl.ds(pl.multiple_of(p % CUTS * height, height), height)]

    def query_copy(r, p):
        to = me - 1 if r == FWD else me + 1
        return remote(piece(q_out, r, p), piece(query_grad, r, p), qs_send.at[r, p], qs_recv.at[r, p], section=to)

    def to_relay(r, p):
        to = me - 2 if r == FWD else me + 2
        slot = p + my_dp * RELAYED[0]
        return remote(piece(q_out, r, p), relay_buf.at[slot], rl_send.at[r, p], rl_recv.at[slot], section=to, dp=n_dp - 1)

    def from_relay(r, d, p):
        to = me + 1 if r == FWD else me - 1
        slot = p + d * RELAYED[0]
        return remote(
            relay_buf.at[slot], piece(query_grad, r, p), rf_send.at[slot], qs_recv.at[r, p], section=to, dp=d
        )

    sends = {FWD: me > 0, REV: me < n_section - 1}
    receives = {FWD: me < n_section - 1, REV: me > 0}
    relays_out = {FWD: me == 2, REV: me == 1}
    last = my_dp == n_dp - 1
    relays_for = {FWD: (me == 0) & last, REV: (me == 3) & last}
    relay_pieces = RELAYED[0] - my_dp * (RELAYED[0] - RELAYED[1])

    def sent_directly(r, do):
        @pl.when(sends[r])
        def _():
            pl.loop(jnp.where(relays_out[r], relay_pieces, 0) if relayed else 0, groups * CUTS)(do)

    def send_queries(r):
        sent_directly(r, lambda p: query_copy(r, p).start())

    def head_copy(r, k):
        to = head_peer(k)
        return remote(
            local.at[r, pl.ds(pl.multiple_of(to * mine, mine), mine)],
            pieces.at[r, k - 1],
            hp_send.at[r, k],
            hp_recv.at[r, k],
            head=to,
        )

    def latent_out(r):
        to = me - 1 if r == FWD else me + 1
        return remote(sums.at[r], latent_grad.at[r, 0], ls_send.at[r], ls_recv.at[r], section=to)

    keys = lax.broadcasted_iota(jnp.int32, (tokens, tokens), 0)
    at = lax.broadcasted_iota(jnp.int32, (tokens, tokens), 1)

    def run(r):
        latents_in(r)
        seg = jnp.broadcast_to(seg_buf[r], (tokens, tokens))
        allowed = (at >= keys) & (seg == jnp.transpose(seg))

        if r == REV and early:
            for first in (0, half):
                load_early(first).wait()
                compute(r, 0, allowed, first, first + half)
        else:
            compute(r, 0, allowed)

        @pl.loop(1, groups)
        def _(g):
            wait_loads(r, g)
            compute(r, g, allowed)

    load_segments.wait()
    rope_sum[...] = jnp.zeros_like(rope_sum)
    if early:
        load_queries(REV, 0).wait()
        load_out(REV, 0).wait()
    else:
        wait_loads(REV, 0)

    @pl.loop(1, groups)
    def _(g):
        start_loads(REV, g)

    load_latents(FWD).start()

    @pl.loop(0, groups)
    def _(g):
        start_loads(FWD, g)

    run(REV)
    load_latents(FWD).wait()
    for k in range(1, n_dp):
        latent_fwd(k).start()
    lt_all[my_dp] = lt_buf[FWD, pl.ds(pl.multiple_of(my_dp * rows, rows), rows), :]
    wait_loads(FWD, 0)
    run(FWD)

    send_queries(FWD)

    for r in (REV, FWD):

        def add(g, total):
            block = kv_rev[g] if r == REV else kv_all[g, slot(my_dp), :]
            return total + dot(block, w_buf[r, g], (1, 1))

        total = lax.fori_loop(0, groups, add, jnp.zeros((tokens, latent), jnp.float32))
        local[r] = jnp.concatenate([total, rope_sum[r]], 1).astype(jnp.bfloat16)
        for k in range(1, n_head):
            head_copy(r, k).start()

    for r in (REV, FWD):
        total = local[r, pl.ds(pl.multiple_of(my_head * mine, mine), mine), :].astype(jnp.float32)
        for k in range(1, n_head):
            head_copy(r, k).wait_recv()
            total += pieces[r, k - 1].astype(jnp.float32)
        sums[r] = total.astype(jnp.bfloat16)

        @pl.when(sends[r])
        def _():
            latent_out(r).start()

    send_queries(REV)

    zeros[...] = jnp.zeros_like(zeros)
    small_zeros[...] = jnp.zeros_like(small_zeros)
    for r in (FWD, REV):

        @pl.when(jnp.logical_not(receives[r]))
        def _():
            for copy in fill(r):
                copy.start()

    @functools.partial(holds_part, my_head)
    def _():
        for k in range(n_dp):
            latent_rev(k).wait_recv()
        for d in range(n_dp):
            for k in range(1, n_head):
                latent_parts(d, k).start()

    if early:
        early_to_mirror(0).wait_recv()
        early_to_mirror(half).wait_recv()
    else:
        kv_to_mirror(0).wait_recv()
    for k in range(1, n_dp):
        kv_passed_on(0, k).start()

    @pl.loop(1, groups)
    def _(g):
        kv_to_mirror(g).wait_recv()
        for k in range(1, n_dp):
            kv_passed_on(g, k).start()

    if relayed:
        for r in (REV, FWD):

            @pl.when(relays_out[r])
            def _():
                pl.loop(0, relay_pieces)(lambda p: to_relay(r, p).start())

    for k in range(1, n_head):

        @functools.partial(holds_part, lax.rem(my_head + n_head - k, n_head))
        def _():
            for d in range(n_dp):
                latent_parts(d, k).wait_recv()

    for k in range(1, n_dp):
        latent_fwd(k).wait_recv()
    latent_rows = jnp.concatenate([lt_all[p] for p in range(2 * n_dp)], 1)

    def put_weight(g):
        return pltpu.make_async_copy(
            w_out.at[g], weight_grad.at[0, :, pl.ds(pl.multiple_of(g * kw, 128), kw)], w_put.at[g]
        )

    @pl.loop(0, groups)
    def _(g):
        for k in range(1, n_dp):
            kv_to_peer(g, k).wait_recv()
            kv_passed_on(g, k).wait_recv()
        w_out[g] = dot(latent_rows, kv_all[g], (1, 0))
        put_weight(g).start()

    if relayed:
        for r in (REV, FWD):

            @pl.when(relays_for[r])
            def _():
                for d in range(n_dp):

                    @pl.loop(0, RELAYED[d])
                    def _(p):
                        arrived = from_relay(r, d, p)
                        remote(relay_buf.at[0], relay_buf.at[0], rf_send.at[0], rl_recv.at[p + d * RELAYED[0]]).wait_recv()
                        arrived.start()

    if early:
        early_to_mirror(0).wait_send()
        early_to_mirror(half).wait_send()
    else:
        kv_to_mirror(0).wait_send()

    @pl.loop(1, groups)
    def _(g):
        kv_to_mirror(g).wait_send()

    @pl.loop(0, groups)
    def _(g):
        put_weight(g).wait()
        for k in range(1, n_dp):
            kv_to_peer(g, k).wait_send()
            kv_passed_on(g, k).wait_send()

    @functools.partial(holds_part, my_head)
    def _():
        for k in range(n_dp):
            latent_rev(k).wait_send()
        for d in range(n_dp):
            for k in range(1, n_head):
                latent_parts(d, k).wait_send()

    for k in range(1, n_dp):
        latent_fwd(k).wait_send()
    for r in (REV, FWD):
        for k in range(1, n_head):
            head_copy(r, k).wait_send()

        @pl.when(jnp.logical_not(receives[r]))
        def _():
            for copy in fill(r):
                copy.wait()

        sent_directly(r, lambda g: query_copy(r, g).wait_send())
        if relayed:

            @pl.when(relays_out[r])
            def _():
                pl.loop(0, relay_pieces)(lambda p: to_relay(r, p).wait_send())

            @pl.when(relays_for[r])
            def _():
                for d in range(n_dp):
                    pl.loop(0, RELAYED[d])(lambda p: from_relay(r, d, p).wait_send())

        @pl.when(sends[r])
        def _():
            latent_out(r).wait_send()

        @pl.when(receives[r])
        def _():
            pl.loop(0, groups * CUTS)(lambda p: query_copy(r, p).wait_recv())
            latent_out(r).wait_recv()


def relay(mesh, queries, latents, out_grad, segment_ids, up_weight):
    n_section, n_dp, n_head = (mesh.shape[a] for a in ("section", "dp", "head"))
    tokens = queries.shape[2]
    latent, width = up_weight.shape[2:]
    features = latents.shape[3]
    heads_here = width // KVDIM
    heads = next(k for k in (GROUP, 2, heads_here) if heads_here % k == 0)
    groups = heads_here // heads
    rows, mine = latent // n_dp, tokens // n_head
    kw = heads * KVDIM
    relayed = n_section == 4 and n_dp == 2 and groups * CUTS > max(RELAYED)
    slots = sum(RELAYED) if relayed else 1
    dma = pltpu.SemaphoreType.DMA
    bf16, f32 = jnp.bfloat16, jnp.float32
    anywhere = pl.BlockSpec(memory_space=pl.ANY)
    args = (queries, jnp.swapaxes(latents, 2, 3), out_grad, segment_ids, up_weight)
    flops = 2 * (2 * tokens * width * latent * 2 + 2 * tokens * tokens * heads_here * 5 * KVDIM)
    return pl.pallas_call(
        functools.partial(relay_kernel, (n_section, n_dp, n_head, heads, groups)),
        in_specs=[anywhere] * 5,
        out_specs=[anywhere] * 3,
        out_shape=[
            jax.ShapeDtypeStruct((2, groups, tokens, heads * QDIM), bf16),
            jax.ShapeDtypeStruct((2, 1, mine, features), bf16),
            jax.ShapeDtypeStruct((1, rows, width), f32),
        ],
        scratch_shapes=[
            pltpu.VMEM((2, groups, tokens, heads * QDIM), bf16),
            pltpu.VMEM((2, features, tokens), bf16),
            pltpu.VMEM((2, groups, tokens, heads * VDIM), bf16),
            pltpu.VMEM((2, groups, latent, kw), bf16),
            pltpu.VMEM((2, tokens, latent), bf16),
            pltpu.VMEM((2, tokens, features - latent), bf16),
            pltpu.VMEM((groups, tokens, kw), bf16),
            pltpu.VMEM((groups, 2 * n_dp * tokens, kw), bf16),
            pltpu.VMEM((2 * n_dp, rows, tokens), bf16),
            pltpu.VMEM((2, groups, tokens, heads * QDIM), bf16),
            pltpu.VMEM((slots, tokens // CUTS, heads * QDIM), bf16),
            pltpu.VMEM((tokens, heads * QDIM), bf16),
            pltpu.VMEM((mine, features), bf16),
            pltpu.VMEM((2, tokens, features), bf16),
            pltpu.VMEM((2, n_head - 1, mine, features), bf16),
            pltpu.VMEM((2, mine, features), bf16),
            pltpu.VMEM((2, tokens, features - latent), f32),
            pltpu.VMEM((groups, rows, kw), f32),
            pltpu.VMEM((2, 1, tokens), jnp.int32),
            dma((2, groups)), dma((2,)), dma((2, groups)), dma((2, groups + 1)), dma((groups,)), dma((groups + 1,)), dma,
            dma((groups + 1,)), dma((groups + 1,)), dma((groups, n_dp)), dma((groups, n_dp)),
            dma((groups, n_dp)), dma((groups, n_dp)), dma((n_dp,)), dma((n_dp,)), dma((n_dp,)), dma((n_dp,)),
            dma((n_dp, n_head)), dma((n_dp, n_head)),
            dma((2, groups * CUTS)), dma((2, groups * CUTS)), dma((2, groups * CUTS)), dma((slots,)), dma((slots,)), dma((2, n_head)), dma((2, n_head)), dma((2,)), dma((2,)),
        ],
        compiler_params=pltpu.CompilerParams(collective_id=0, has_side_effects=True, vmem_limit_bytes=44 << 20),
        cost_estimate=pl.CostEstimate(flops=flops, bytes_accessed=8 * latent * width, transcendentals=0),
        name="relay",
    )(*(pltpu.with_memory_space_constraint(x, pltpu.HBM) for x in args))


def unload_kernel(arrived, latent_in, weight_in, query_grad, latent_grad, weight_grad, sem, query_sem, weight_sem):
    groups, width = arrived.shape[1], arrived.shape[3]
    blocks = weight_sem.shape[0]
    rows = weight_in.shape[1] // blocks
    copies = (
        [
            pltpu.make_async_copy(
                weight_in.at[:, pl.ds(b * rows, rows)], weight_grad.at[:, pl.ds(b * rows, rows)], weight_sem.at[b]
            )
            for b in range(blocks)
        ]
        + [
            pltpu.make_async_copy(arrived.at[r, g], query_grad.at[r, 0, :, pl.ds(g * width, width)], query_sem.at[r, g])
            for r in (FWD, REV)
            for g in range(groups)
        ]
        + [pltpu.make_async_copy(latent_in, latent_grad, sem)]
    )
    for copy in copies:
        copy.start()
    for copy in copies:
        copy.wait()


def unload(arrived, latent_grad, weight_grad):
    two, groups, tokens, width = arrived.shape
    blocks = next(b for b in (BLOCKS, 2, 1) if weight_grad.shape[1] % (8 * b) == 0)
    anywhere = pl.BlockSpec(memory_space=pl.ANY)
    dma = pltpu.SemaphoreType.DMA
    return pl.pallas_call(
        unload_kernel,
        in_specs=[anywhere] * 3,
        out_specs=[anywhere] * 3,
        out_shape=[
            pltpu.HBM((two, 1, tokens, groups * width), arrived.dtype),
            pltpu.HBM(latent_grad.shape, latent_grad.dtype),
            pltpu.HBM(weight_grad.shape, weight_grad.dtype),
        ],
        scratch_shapes=[dma, dma((two, groups)), dma((blocks,))],
        compiler_params=pltpu.CompilerParams(vmem_limit_bytes=1 << 20),
        name="unload",
    )(arrived, latent_grad, weight_grad)


def solution(mesh):
    in_specs = (
        P(None, "section", "dp", "head"),
        P(None, "section", "dp", None),
        P(None, "section", "dp", "head"),
        P(None, "section", "dp"),
        P(None, "section", None, "head"),
    )
    out_specs = (
        P(None, "section", "dp", "head"),
        P(None, "section", ("dp", "head"), None),
        P("section", "dp", "head"),
    )
    def body(*args):
        return unload(*relay(mesh, *args))

    return jax.shard_map(body, mesh=mesh, in_specs=in_specs, out_specs=out_specs, check_vma=False)
```

```python
import functools

import jax
import jax.numpy as jnp
from jax import lax
from jax.experimental import pallas as pl
from jax.experimental.pallas import tpu as pltpu
from jax.sharding import PartitionSpec as P

ROPE = 64
NOPE = 128
VDIM = 128
QDIM = NOPE + ROPE
KVDIM = NOPE + VDIM
GROUP = 4
CUTS = 4
BLOCKS = 1
RELAYED = (10, 7)
FWD, REV = 0, 1
MESH = pl.DeviceIdType.MESH


def dot(a, b, contract):
    return lax.dot_general(a, b, ((contract[:1], contract[1:]), ((), ())), preferred_element_type=jnp.float32)


def relay_kernel(
    sizes,
    queries, latents_t, out_grad, segments, weight,
    query_grad, latent_grad, weight_grad,
    q_buf, lt_buf, o_buf, w_buf, lat, rope, kv_rev, kv_all, lt_all, q_out, relay_buf, zeros, small_zeros,
    local, pieces, sums, rope_sum, w_out, seg_buf,
    q_in, lt_in, o_in, w_in, w_put, z_put, seg_in,
    kr_send, kr_recv, kf_send, kf_recv, kx_send, kx_recv, lr_send, lr_recv, lf_send, lf_recv, lx_send, lx_recv,
    qs_send, qs_recv, rl_send, rl_recv, rf_send, hp_send, hp_recv, ls_send, ls_recv,
):
    n_section, n_dp, n_head, heads, groups = sizes
    me, my_dp, my_head = lax.axis_index("section"), lax.axis_index("dp"), lax.axis_index("head")
    mirror = n_section - 1 - me
    tokens = queries.shape[2]
    latent = weight.shape[2]
    rows = latent // n_dp
    mine = tokens // n_head
    parts = min(n_head, rows // 16)
    part = rows // parts
    kw, qw, ow = heads * KVDIM, heads * QDIM, heads * VDIM
    relayed = relay_buf.shape[0] > 1
    height = tokens // CUTS
    scale = QDIM ** (-0.5)

    def remote(src, dst, send, recv, **where):
        return pltpu.make_async_remote_copy(
            src_ref=src, dst_ref=dst, send_sem=send, recv_sem=recv, device_id=where, device_id_type=MESH
        )

    def dp_peer(k):
        return lax.rem(my_dp + k, n_dp)

    def load_weight(r, g):
        cols = pl.ds(pl.multiple_of(g * kw, 128), kw)
        return pltpu.make_async_copy(weight.at[r, 0, :, cols], w_buf.at[r, g], w_in.at[r, g])

    half = heads // 2
    early = heads % 4 == 0

    def load_early(first):
        cols = pl.ds(first * KVDIM, half * KVDIM)
        return pltpu.make_async_copy(
            weight.at[REV, 0, :, cols], w_buf.at[REV, 0, :, cols], w_in.at[REV, groups * min(first, 1)]
        )

    def load_latents(r):
        return pltpu.make_async_copy(latents_t.at[r, 0], lt_buf.at[r], lt_in.at[r])

    def load_queries(r, g):
        cols = pl.ds(pl.multiple_of(g * qw, 128), qw)
        return pltpu.make_async_copy(queries.at[r, 0, :, cols], q_buf.at[r, g], q_in.at[r, g])

    def load_out(r, g):
        cols = pl.ds(pl.multiple_of(g * ow, 128), ow)
        return pltpu.make_async_copy(out_grad.at[r, 0, :, cols], o_buf.at[r, g], o_in.at[r, g])

    def start_loads(r, g):
        load_weight(r, g).start()
        load_queries(r, g).start()
        load_out(r, g).start()

    def wait_loads(r, g):
        load_weight(r, g).wait()
        load_queries(r, g).wait()
        load_out(r, g).wait()

    has_left, has_right = jnp.where(my_head > 0, 1, 0), jnp.where(my_head < n_head - 1, 1, 0)
    barrier = pltpu.get_barrier_semaphore()
    for k in range(1, n_section):
        pl.semaphore_signal(barrier, 1, device_id={"section": lax.rem(me + k, n_section)}, device_id_type=MESH)
    for k in range(1, n_dp):
        pl.semaphore_signal(barrier, 1, device_id={"dp": dp_peer(k)}, device_id_type=MESH)
        for section in [lax.rem(me + j, n_section) for j in range(1, n_section)] if relayed else [mirror]:
            pl.semaphore_signal(barrier, 1, device_id={"section": section, "dp": dp_peer(k)}, device_id_type=MESH)
    for step in (-1, 1):

        @pl.when((my_head + step >= 0) & (my_head + step < n_head))
        def _():
            pl.semaphore_signal(barrier, 1, device_id={"head": my_head + step}, device_id_type=MESH)


    load_segments = pltpu.make_async_copy(segments, seg_buf, seg_in)
    load_latents(REV).start()
    if early:
        load_early(0).start()
        load_queries(REV, 0).start()
        load_out(REV, 0).start()
        load_early(half).start()
    else:
        start_loads(REV, 0)
    load_segments.start()

    def latents_in(r):
        lat[r] = jnp.transpose(lt_buf[r, :latent, :].astype(jnp.float32)).astype(jnp.bfloat16)
        rope[r] = jnp.transpose(lt_buf[r, latent:, :].astype(jnp.float32)).astype(jnp.bfloat16)

    load_latents(REV).wait()
    pl.semaphore_wait(barrier, n_section - 1 + (n_section if relayed else 2) * (n_dp - 1) + has_left + has_right)

    def latent_rev(k):
        to = dp_peer(k)
        block = pl.ds(pl.multiple_of(to * rows + my_head * part, part), part)
        return remote(
            lt_buf.at[REV, block],
            lt_all.at[n_dp + my_dp, pl.ds(pl.multiple_of(my_head * part, part), part)],
            lr_send.at[k],
            lr_recv.at[k],
            section=mirror,
            dp=to,
        )

    def latent_fwd(k):
        to = dp_peer(k)
        block = pl.ds(pl.multiple_of(to * rows, rows), rows)
        return remote(lt_buf.at[FWD, block], lt_all.at[my_dp], lf_send.at[k], lf_recv.at[k], dp=to)

    def latent_part(d, j, way):
        ref = lt_all.at[n_dp + d, pl.ds(pl.multiple_of(j * part, part), part)]
        side = (way + 1) // 2
        return remote(ref, ref, lx_send.at[d, side, j], lx_recv.at[d, side, j], head=my_head + way)

    def pass_parts(way, do):
        low, high = (0, jnp.minimum(my_head + 1, parts)) if way > 0 else (my_head, parts)
        return pl.loop(low, high)(do)

    def holds_part(head, do):
        if parts == n_head:
            do()
        else:
            pl.when(head < parts)(do)

    @functools.partial(holds_part, my_head)
    def _():
        for k in range(n_dp):
            latent_rev(k).start()

    def fill(r):
        return [
            pltpu.make_async_copy(zeros, query_grad.at[r, g], z_put.at[g]) for g in range(groups)
        ] + [pltpu.make_async_copy(small_zeros, latent_grad.at[r, 0], z_put.at[groups])]

    def slot(piece):
        return pl.ds(pl.multiple_of(piece * tokens, tokens), tokens)

    def kv_to_mirror(g):
        return remote(kv_rev.at[g], kv_all.at[g, slot(n_dp + my_dp)], kr_send.at[g], kr_recv.at[g], section=mirror)

    def early_to_mirror(first):
        cols, sem = pl.ds(first * KVDIM, half * KVDIM), groups * min(first, 1)
        return remote(
            kv_rev.at[0, :, cols], kv_all.at[0, slot(n_dp + my_dp), cols], kr_send.at[sem], kr_recv.at[sem], section=mirror
        )

    def kv_to_peer(g, k):
        ref = kv_all.at[g, slot(my_dp)]
        return remote(ref, ref, kf_send.at[g, k], kf_recv.at[g, k], dp=dp_peer(k))

    def kv_passed_on(g, k):
        ref = kv_all.at[g, slot(n_dp + my_dp)]
        return remote(ref, ref, kx_send.at[g, k], kx_recv.at[g, k], dp=dp_peer(k))

    def compute(r, g, allowed, first=0, end=heads):
        kv = dot(lat[r], w_buf[r, g, :, first * KVDIM : end * KVDIM], (1, 0)).astype(jnp.bfloat16)
        query_block = q_buf[r, g, :, first * QDIM : end * QDIM]
        out_block = o_buf[r, g, :, first * VDIM : end * VDIM]
        key_rope = rope[r]
        query_parts, kv_parts = [], []
        total = rope_sum[r]
        for h in range(end - first):
            key = jnp.concatenate([kv[:, h * KVDIM : h * KVDIM + NOPE], key_rope], 1)
            value = kv[:, h * KVDIM + NOPE : (h + 1) * KVDIM]
            query = query_block[:, h * QDIM : (h + 1) * QDIM]
            out = out_block[:, h * VDIM : (h + 1) * VDIM]
            scores = jnp.where(allowed, dot(key, query, (1, 1)) * scale, jnp.float32(-1e30))
            powers = jnp.exp(scores - jnp.max(scores, axis=0, keepdims=True))
            probs = powers * (1.0 / jnp.sum(powers, axis=0, keepdims=True))
            grad_probs = dot(value, out, (1, 1))
            delta = jnp.sum(probs * grad_probs, axis=0, keepdims=True)
            score_grad = (probs * (grad_probs - delta) * scale).astype(jnp.bfloat16)
            value_grad = dot(probs.astype(jnp.bfloat16), out, (1, 0))
            key_grad = dot(score_grad, query, (1, 0))
            total += key_grad[:, NOPE:]
            query_parts.append(dot(score_grad, key, (0, 0)))
            kv_parts += [key_grad[:, :NOPE].astype(jnp.bfloat16), value_grad.astype(jnp.bfloat16)]
        rope_sum[r] = total
        q_out[r, g, :, first * QDIM : end * QDIM] = jnp.concatenate(query_parts, 1).astype(jnp.bfloat16)
        kv_out = jnp.concatenate(kv_parts, 1)
        if r == REV:
            kv_rev[g, :, first * KVDIM : end * KVDIM] = kv_out
            (kv_to_mirror(g) if end - first == heads else early_to_mirror(first)).start()
        else:
            kv_all[g, slot(my_dp), :] = kv_out
            for k in range(1, n_dp):
                kv_to_peer(g, k).start()

    def piece(ref, r, p):
        return ref.at[r, p // CUTS, pl.ds(pl.multiple_of(p % CUTS * height, height), height)]

    def query_copy(r, p):
        to = me - 1 if r == FWD else me + 1
        return remote(piece(q_out, r, p), piece(query_grad, r, p), qs_send.at[r, p], qs_recv.at[r, p], section=to)

    def to_relay(r, p):
        to = me - 2 if r == FWD else me + 2
        slot = p + my_dp * RELAYED[0]
        return remote(piece(q_out, r, p), relay_buf.at[slot], rl_send.at[r, p], rl_recv.at[slot], section=to, dp=n_dp - 1)

    def from_relay(r, d, p):
        to = me + 1 if r == FWD else me - 1
        slot = p + d * RELAYED[0]
        return remote(
            relay_buf.at[slot], piece(query_grad, r, p), rf_send.at[slot], qs_recv.at[r, p], section=to, dp=d
        )

    sends = {FWD: me > 0, REV: me < n_section - 1}
    receives = {FWD: me < n_section - 1, REV: me > 0}
    relays_out = {FWD: me == 2, REV: me == 1}
    last = my_dp == n_dp - 1
    relays_for = {FWD: (me == 0) & last, REV: (me == 3) & last}
    relay_pieces = RELAYED[0] - my_dp * (RELAYED[0] - RELAYED[1])

    def sent_directly(r, do):
        @pl.when(sends[r])
        def _():
            pl.loop(jnp.where(relays_out[r], relay_pieces, 0) if relayed else 0, groups * CUTS)(do)

    def send_queries(r):
        sent_directly(r, lambda p: query_copy(r, p).start())

    def head_copy(r, d, way):
        side = (way + 1) // 2
        ref = pieces.at[r, side, d]
        return remote(ref, ref, hp_send.at[r, side, d], hp_recv.at[r, side, d], head=my_head + way)

    def further(way, do):
        return pl.loop(my_head + 1, n_head)(do) if way > 0 else pl.loop(0, my_head)(do)

    def sum_on(way):
        side = (way + 1) // 2
        behind = has_left if way > 0 else has_right

        for r in (REV, FWD):

            def do(d):
                @pl.when(behind == 1)
                def _():
                    head_copy(r, d, way).wait_recv()
                    total = local[r, d] + pieces[r, side, d].astype(jnp.float32)
                    pieces[r, side, d] = total.astype(jnp.bfloat16)

                @pl.when(behind == 0)
                def _():
                    pieces[r, side, d] = local[r, d].astype(jnp.bfloat16)

                head_copy(r, d, way).start()

            further(way, do)

        @pl.when(behind == 1)
        def _():
            for r in (REV, FWD):
                head_copy(r, my_head, way).wait_recv()
                local[r, my_head] += pieces[r, side, my_head].astype(jnp.float32)

    def both_ways(do):
        @pl.when(my_head < n_head // 2)
        def _():
            do(1)
            do(-1)

        @pl.when(my_head >= n_head // 2)
        def _():
            do(-1)
            do(1)

    def latent_out(r):
        to = me - 1 if r == FWD else me + 1
        return remote(sums.at[r], latent_grad.at[r, 0], ls_send.at[r], ls_recv.at[r], section=to)

    keys = lax.broadcasted_iota(jnp.int32, (tokens, tokens), 0)
    at = lax.broadcasted_iota(jnp.int32, (tokens, tokens), 1)

    def run(r):
        latents_in(r)
        seg = jnp.broadcast_to(seg_buf[r], (tokens, tokens))
        allowed = (at >= keys) & (seg == jnp.transpose(seg))

        if r == REV and early:
            for first in (0, half):
                load_early(first).wait()
                compute(r, 0, allowed, first, first + half)
        else:
            compute(r, 0, allowed)

        @pl.loop(1, groups)
        def _(g):
            wait_loads(r, g)
            compute(r, g, allowed)

    load_segments.wait()
    rope_sum[...] = jnp.zeros_like(rope_sum)
    if early:
        load_queries(REV, 0).wait()
        load_out(REV, 0).wait()
    else:
        wait_loads(REV, 0)

    @pl.loop(1, groups)
    def _(g):
        start_loads(REV, g)

    load_latents(FWD).start()

    @pl.loop(0, groups)
    def _(g):
        start_loads(FWD, g)

    run(REV)
    load_latents(FWD).wait()
    for k in range(1, n_dp):
        latent_fwd(k).start()
    lt_all[my_dp] = lt_buf[FWD, pl.ds(pl.multiple_of(my_dp * rows, rows), rows), :]
    wait_loads(FWD, 0)
    run(FWD)

    send_queries(FWD)
    pl.when(me == 0)(lambda: send_queries(REV))

    for r in (REV, FWD):

        def add(g, total):
            block = kv_rev[g] if r == REV else kv_all[g, slot(my_dp), :]
            return total + dot(block, w_buf[r, g], (1, 1))

        total = lax.fori_loop(0, groups, add, jnp.zeros((tokens, latent), jnp.float32))
        local[r] = jnp.concatenate([total, rope_sum[r]], 1).reshape(n_head, mine, total.shape[1] + rope_sum.shape[2])

    both_ways(sum_on)
    for r in (REV, FWD):
        sums[r] = local[r, my_head].astype(jnp.bfloat16)

        @pl.when(sends[r])
        def _():
            latent_out(r).start()

    pl.when(me > 0)(lambda: send_queries(REV))

    zeros[...] = jnp.zeros_like(zeros)
    small_zeros[...] = jnp.zeros_like(small_zeros)
    for r in (FWD, REV):

        @pl.when(jnp.logical_not(receives[r]))
        def _():
            for copy in fill(r):
                copy.start()

    @functools.partial(holds_part, my_head)
    def _():
        for k in range(n_dp):
            latent_rev(k).wait_recv()

    def pass_on(way):
        def do(j):
            for d in range(n_dp):
                pl.when(j != my_head)(lambda: latent_part(d, j, way).wait_recv())
                pl.when((has_right if way > 0 else has_left) == 1)(lambda: latent_part(d, j, way).start())

        pass_parts(way, do)

    both_ways(pass_on)

    if early:
        early_to_mirror(0).wait_recv()
        early_to_mirror(half).wait_recv()
    else:
        kv_to_mirror(0).wait_recv()
    for k in range(1, n_dp):
        kv_passed_on(0, k).start()

    @pl.loop(1, groups)
    def _(g):
        kv_to_mirror(g).wait_recv()
        for k in range(1, n_dp):
            kv_passed_on(g, k).start()

    if relayed:
        for r in (REV, FWD):

            @pl.when(relays_out[r])
            def _():
                pl.loop(0, relay_pieces)(lambda p: to_relay(r, p).start())

    if relayed:
        for r in (REV, FWD):

            @pl.when(relays_for[r])
            def _():
                for d in range(n_dp):

                    @pl.loop(0, RELAYED[d])
                    def _(p):
                        arrived = from_relay(r, d, p)
                        remote(relay_buf.at[0], relay_buf.at[0], rf_send.at[0], rl_recv.at[p + d * RELAYED[0]]).wait_recv()
                        arrived.start()

    for k in range(1, n_dp):
        latent_fwd(k).wait_recv()
    latent_rows = jnp.concatenate([lt_all[p] for p in range(2 * n_dp)], 1)

    def put_weight(g):
        return pltpu.make_async_copy(
            w_out.at[g], weight_grad.at[0, :, pl.ds(pl.multiple_of(g * kw, 128), kw)], w_put.at[g]
        )

    @pl.loop(0, groups)
    def _(g):
        for k in range(1, n_dp):
            kv_to_peer(g, k).wait_recv()
            kv_passed_on(g, k).wait_recv()
        w_out[g] = dot(latent_rows, kv_all[g], (1, 0))
        put_weight(g).start()

    if early:
        early_to_mirror(0).wait_send()
        early_to_mirror(half).wait_send()
    else:
        kv_to_mirror(0).wait_send()

    @pl.loop(1, groups)
    def _(g):
        kv_to_mirror(g).wait_send()

    @pl.loop(0, groups)
    def _(g):
        put_weight(g).wait()
        for k in range(1, n_dp):
            kv_to_peer(g, k).wait_send()
            kv_passed_on(g, k).wait_send()

    @functools.partial(holds_part, my_head)
    def _():
        for k in range(n_dp):
            latent_rev(k).wait_send()

    for way, there in ((1, has_right), (-1, has_left)):

        @pl.when(there == 1)
        def _():
            def sent(j):
                for d in range(n_dp):
                    latent_part(d, j, way).wait_send()

            pass_parts(way, sent)

    for k in range(1, n_dp):
        latent_fwd(k).wait_send()
    for r in (REV, FWD):
        for way in (1, -1):
            further(way, lambda d: head_copy(r, d, way).wait_send())

        @pl.when(jnp.logical_not(receives[r]))
        def _():
            for copy in fill(r):
                copy.wait()

        sent_directly(r, lambda g: query_copy(r, g).wait_send())
        if relayed:

            @pl.when(relays_out[r])
            def _():
                pl.loop(0, relay_pieces)(lambda p: to_relay(r, p).wait_send())

            @pl.when(relays_for[r])
            def _():
                for d in range(n_dp):
                    pl.loop(0, RELAYED[d])(lambda p: from_relay(r, d, p).wait_send())

        @pl.when(sends[r])
        def _():
            latent_out(r).wait_send()

        @pl.when(receives[r])
        def _():
            pl.loop(0, groups * CUTS)(lambda p: query_copy(r, p).wait_recv())
            latent_out(r).wait_recv()


def relay(mesh, queries, latents, out_grad, segment_ids, up_weight):
    n_section, n_dp, n_head = (mesh.shape[a] for a in ("section", "dp", "head"))
    tokens = queries.shape[2]
    latent, width = up_weight.shape[2:]
    features = latents.shape[3]
    heads_here = width // KVDIM
    heads = next(k for k in (GROUP, 2, heads_here) if heads_here % k == 0)
    groups = heads_here // heads
    rows, mine = latent // n_dp, tokens // n_head
    kw = heads * KVDIM
    relayed = n_section == 4 and n_dp == 2 and groups * CUTS > max(RELAYED)
    slots = sum(RELAYED) if relayed else 1
    dma = pltpu.SemaphoreType.DMA
    bf16, f32 = jnp.bfloat16, jnp.float32
    anywhere = pl.BlockSpec(memory_space=pl.ANY)
    args = (queries, jnp.swapaxes(latents, 2, 3), out_grad, segment_ids, up_weight)
    flops = 2 * (2 * tokens * width * latent * 2 + 2 * tokens * tokens * heads_here * 5 * KVDIM)
    return pl.pallas_call(
        functools.partial(relay_kernel, (n_section, n_dp, n_head, heads, groups)),
        in_specs=[anywhere] * 5,
        out_specs=[anywhere] * 3,
        out_shape=[
            jax.ShapeDtypeStruct((2, groups, tokens, heads * QDIM), bf16),
            jax.ShapeDtypeStruct((2, 1, mine, features), bf16),
            jax.ShapeDtypeStruct((1, rows, width), f32),
        ],
        scratch_shapes=[
            pltpu.VMEM((2, groups, tokens, heads * QDIM), bf16),
            pltpu.VMEM((2, features, tokens), bf16),
            pltpu.VMEM((2, groups, tokens, heads * VDIM), bf16),
            pltpu.VMEM((2, groups, latent, kw), bf16),
            pltpu.VMEM((2, tokens, latent), bf16),
            pltpu.VMEM((2, tokens, features - latent), bf16),
            pltpu.VMEM((groups, tokens, kw), bf16),
            pltpu.VMEM((groups, 2 * n_dp * tokens, kw), bf16),
            pltpu.VMEM((2 * n_dp, rows, tokens), bf16),
            pltpu.VMEM((2, groups, tokens, heads * QDIM), bf16),
            pltpu.VMEM((slots, tokens // CUTS, heads * QDIM), bf16),
            pltpu.VMEM((tokens, heads * QDIM), bf16),
            pltpu.VMEM((mine, features), bf16),
            pltpu.VMEM((2, n_head, mine, features), f32),
            pltpu.VMEM((2, 2, n_head, mine, features), bf16),
            pltpu.VMEM((2, mine, features), bf16),
            pltpu.VMEM((2, tokens, features - latent), f32),
            pltpu.VMEM((groups, rows, kw), f32),
            pltpu.VMEM((2, 1, tokens), jnp.int32),
            dma((2, groups)), dma((2,)), dma((2, groups)), dma((2, groups + 1)), dma((groups,)), dma((groups + 1,)), dma,
            dma((groups + 1,)), dma((groups + 1,)), dma((groups, n_dp)), dma((groups, n_dp)),
            dma((groups, n_dp)), dma((groups, n_dp)), dma((n_dp,)), dma((n_dp,)), dma((n_dp,)), dma((n_dp,)),
            dma((n_dp, 2, n_head)), dma((n_dp, 2, n_head)),
            dma((2, groups * CUTS)), dma((2, groups * CUTS)), dma((2, groups * CUTS)), dma((slots,)), dma((slots,)), dma((2, 2, n_head)), dma((2, 2, n_head)), dma((2,)), dma((2,)),
        ],
        compiler_params=pltpu.CompilerParams(collective_id=0, has_side_effects=True, vmem_limit_bytes=44 << 20),
        cost_estimate=pl.CostEstimate(flops=flops, bytes_accessed=8 * latent * width, transcendentals=0),
        name="relay",
    )(*(pltpu.with_memory_space_constraint(x, pltpu.HBM) for x in args))


def unload_kernel(arrived, latent_in, weight_in, query_grad, latent_grad, weight_grad, sem, query_sem, weight_sem):
    groups, width = arrived.shape[1], arrived.shape[3]
    blocks = weight_sem.shape[0]
    rows = weight_in.shape[1] // blocks
    copies = (
        [
            pltpu.make_async_copy(
                weight_in.at[:, pl.ds(b * rows, rows)], weight_grad.at[:, pl.ds(b * rows, rows)], weight_sem.at[b]
            )
            for b in range(blocks)
        ]
        + [
            pltpu.make_async_copy(arrived.at[r, g], query_grad.at[r, 0, :, pl.ds(g * width, width)], query_sem.at[r, g])
            for r in (FWD, REV)
            for g in range(groups)
        ]
        + [pltpu.make_async_copy(latent_in, latent_grad, sem)]
    )
    for copy in copies:
        copy.start()
    for copy in copies:
        copy.wait()


def unload(arrived, latent_grad, weight_grad):
    two, groups, tokens, width = arrived.shape
    blocks = next(b for b in (BLOCKS, 2, 1) if weight_grad.shape[1] % (8 * b) == 0)
    anywhere = pl.BlockSpec(memory_space=pl.ANY)
    dma = pltpu.SemaphoreType.DMA
    return pl.pallas_call(
        unload_kernel,
        in_specs=[anywhere] * 3,
        out_specs=[anywhere] * 3,
        out_shape=[
            pltpu.HBM((two, 1, tokens, groups * width), arrived.dtype),
            pltpu.HBM(latent_grad.shape, latent_grad.dtype),
            pltpu.HBM(weight_grad.shape, weight_grad.dtype),
        ],
        scratch_shapes=[dma, dma((two, groups)), dma((blocks,))],
        compiler_params=pltpu.CompilerParams(vmem_limit_bytes=1 << 20),
        name="unload",
    )(arrived, latent_grad, weight_grad)


def solution(mesh):
    in_specs = (
        P(None, "section", "dp", "head"),
        P(None, "section", "dp", None),
        P(None, "section", "dp", "head"),
        P(None, "section", "dp"),
        P(None, "section", None, "head"),
    )
    out_specs = (
        P(None, "section", "dp", "head"),
        P(None, "section", ("dp", "head"), None),
        P("section", "dp", "head"),
    )
    def body(*args):
        return unload(*relay(mesh, *args))

    return jax.shard_map(body, mesh=mesh, in_specs=in_specs, out_specs=out_specs, check_vma=False)
```

```python
import functools

import jax
import jax.numpy as jnp
from jax import lax
from jax.experimental import pallas as pl
from jax.experimental.pallas import tpu as pltpu
from jax.sharding import PartitionSpec as P

ROPE = 64
NOPE = 128
VDIM = 128
QDIM = NOPE + ROPE
KVDIM = NOPE + VDIM
GROUP = 4
CUTS = 2
BLOCKS = 1
RELAYED = (5, 3)
FWD, REV = 0, 1
MESH = pl.DeviceIdType.MESH


def dot(a, b, contract):
    return lax.dot_general(a, b, ((contract[:1], contract[1:]), ((), ())), preferred_element_type=jnp.float32)


def relay_kernel(
    sizes,
    queries, latents_t, out_grad, segments, weight,
    query_grad, latent_grad, weight_grad,
    q_buf, lt_buf, o_buf, w_buf, lat, rope, kv_rev, kv_all, lt_all, q_out, relay_buf, zeros, small_zeros,
    local, pieces, sums, rope_sum, w_out, seg_buf,
    q_in, lt_in, o_in, w_in, w_put, z_put, seg_in,
    kr_send, kr_recv, kf_send, kf_recv, kx_send, kx_recv, lr_send, lr_recv, lf_send, lf_recv, lx_send, lx_recv,
    qs_send, qs_recv, rl_send, rl_recv, rf_send, hp_send, hp_recv, ls_send, ls_recv,
):
    n_section, n_dp, n_head, heads, groups = sizes
    me, my_dp, my_head = lax.axis_index("section"), lax.axis_index("dp"), lax.axis_index("head")
    mirror = n_section - 1 - me
    tokens = queries.shape[2]
    latent = weight.shape[2]
    rows = latent // n_dp
    mine = tokens // n_head
    parts = min(n_head, rows // 16)
    part = rows // parts
    kw, qw, ow = heads * KVDIM, heads * QDIM, heads * VDIM
    relayed = relay_buf.shape[0] > 1
    height = tokens // CUTS
    scale = QDIM ** (-0.5)

    def remote(src, dst, send, recv, **where):
        return pltpu.make_async_remote_copy(
            src_ref=src, dst_ref=dst, send_sem=send, recv_sem=recv, device_id=where, device_id_type=MESH
        )

    def dp_peer(k):
        return lax.rem(my_dp + k, n_dp)

    def load_weight(r, g):
        cols = pl.ds(pl.multiple_of(g * kw, 128), kw)
        return pltpu.make_async_copy(weight.at[r, 0, :, cols], w_buf.at[r, g], w_in.at[r, g])

    half = heads // 2
    early = heads % 4 == 0

    def load_early(first):
        cols = pl.ds(first * KVDIM, half * KVDIM)
        return pltpu.make_async_copy(
            weight.at[REV, 0, :, cols], w_buf.at[REV, 0, :, cols], w_in.at[REV, groups * min(first, 1)]
        )

    def load_latents(r):
        return pltpu.make_async_copy(latents_t.at[r, 0], lt_buf.at[r], lt_in.at[r])

    def load_queries(r, g):
        cols = pl.ds(pl.multiple_of(g * qw, 128), qw)
        return pltpu.make_async_copy(queries.at[r, 0, :, cols], q_buf.at[r, g], q_in.at[r, g])

    def load_out(r, g):
        cols = pl.ds(pl.multiple_of(g * ow, 128), ow)
        return pltpu.make_async_copy(out_grad.at[r, 0, :, cols], o_buf.at[r, g], o_in.at[r, g])

    def start_loads(r, g):
        load_weight(r, g).start()
        load_queries(r, g).start()
        load_out(r, g).start()

    def wait_loads(r, g):
        load_weight(r, g).wait()
        load_queries(r, g).wait()
        load_out(r, g).wait()

    has_left, has_right = jnp.where(my_head > 0, 1, 0), jnp.where(my_head < n_head - 1, 1, 0)
    barrier = pltpu.get_barrier_semaphore()
    for k in range(1, n_section):
        pl.semaphore_signal(barrier, 1, device_id={"section": lax.rem(me + k, n_section)}, device_id_type=MESH)
    for k in range(1, n_dp):
        pl.semaphore_signal(barrier, 1, device_id={"dp": dp_peer(k)}, device_id_type=MESH)
        for section in [lax.rem(me + j, n_section) for j in range(1, n_section)] if relayed else [mirror]:
            pl.semaphore_signal(barrier, 1, device_id={"section": section, "dp": dp_peer(k)}, device_id_type=MESH)
    for step in (-1, 1):

        @pl.when((my_head + step >= 0) & (my_head + step < n_head))
        def _():
            pl.semaphore_signal(barrier, 1, device_id={"head": my_head + step}, device_id_type=MESH)


    load_segments = pltpu.make_async_copy(segments, seg_buf, seg_in)
    load_latents(REV).start()
    if early:
        load_early(0).start()
        load_queries(REV, 0).start()
        load_out(REV, 0).start()
        load_early(half).start()
    else:
        start_loads(REV, 0)
    load_segments.start()

    def latents_in(r):
        lat[r] = jnp.transpose(lt_buf[r, :latent, :].astype(jnp.float32)).astype(jnp.bfloat16)
        rope[r] = jnp.transpose(lt_buf[r, latent:, :].astype(jnp.float32)).astype(jnp.bfloat16)

    load_latents(REV).wait()
    pl.semaphore_wait(barrier, n_section - 1 + (n_section if relayed else 2) * (n_dp - 1) + has_left + has_right)

    def latent_rev(k):
        to = dp_peer(k)
        block = pl.ds(pl.multiple_of(to * rows + my_head * part, part), part)
        return remote(
            lt_buf.at[REV, block],
            lt_all.at[n_dp + my_dp, pl.ds(pl.multiple_of(my_head * part, part), part)],
            lr_send.at[k],
            lr_recv.at[k],
            section=mirror,
            dp=to,
        )

    def latent_fwd(k):
        to = dp_peer(k)
        block = pl.ds(pl.multiple_of(to * rows, rows), rows)
        return remote(lt_buf.at[FWD, block], lt_all.at[my_dp], lf_send.at[k], lf_recv.at[k], dp=to)

    def latent_part(d, j, way):
        ref = lt_all.at[n_dp + d, pl.ds(pl.multiple_of(j * part, part), part)]
        side = (way + 1) // 2
        return remote(ref, ref, lx_send.at[d, side, j], lx_recv.at[d, side, j], head=my_head + way)

    def pass_parts(way, do):
        low, high = (0, jnp.minimum(my_head + 1, parts)) if way > 0 else (my_head, parts)
        return pl.loop(low, high)(do)

    def holds_part(head, do):
        if parts == n_head:
            do()
        else:
            pl.when(head < parts)(do)

    @functools.partial(holds_part, my_head)
    def _():
        for k in range(n_dp):
            latent_rev(k).start()

    def fill(r):
        return [
            pltpu.make_async_copy(zeros, query_grad.at[r, g], z_put.at[g]) for g in range(groups)
        ] + [pltpu.make_async_copy(small_zeros, latent_grad.at[r, 0], z_put.at[groups])]

    def slot(piece):
        return pl.ds(pl.multiple_of(piece * tokens, tokens), tokens)

    def kv_to_mirror(g):
        return remote(kv_rev.at[g], kv_all.at[g, slot(n_dp + my_dp)], kr_send.at[g], kr_recv.at[g], section=mirror)

    def early_to_mirror(first):
        cols, sem = pl.ds(first * KVDIM, half * KVDIM), groups * min(first, 1)
        return remote(
            kv_rev.at[0, :, cols], kv_all.at[0, slot(n_dp + my_dp), cols], kr_send.at[sem], kr_recv.at[sem], section=mirror
        )

    def kv_to_peer(g, k):
        ref = kv_all.at[g, slot(my_dp)]
        return remote(ref, ref, kf_send.at[g, k], kf_recv.at[g, k], dp=dp_peer(k))

    def kv_passed_on(g, k):
        ref = kv_all.at[g, slot(n_dp + my_dp)]
        return remote(ref, ref, kx_send.at[g, k], kx_recv.at[g, k], dp=dp_peer(k))

    def compute(r, g, allowed, first=0, end=heads):
        kv = dot(lat[r], w_buf[r, g, :, first * KVDIM : end * KVDIM], (1, 0)).astype(jnp.bfloat16)
        query_block = q_buf[r, g, :, first * QDIM : end * QDIM]
        out_block = o_buf[r, g, :, first * VDIM : end * VDIM]
        key_rope = rope[r]
        query_parts, kv_parts = [], []
        total = rope_sum[r]
        for h in range(end - first):
            key = jnp.concatenate([kv[:, h * KVDIM : h * KVDIM + NOPE], key_rope], 1)
            value = kv[:, h * KVDIM + NOPE : (h + 1) * KVDIM]
            query = query_block[:, h * QDIM : (h + 1) * QDIM]
            out = out_block[:, h * VDIM : (h + 1) * VDIM]
            scores = jnp.where(allowed, dot(key, query, (1, 1)) * scale, jnp.float32(-1e30))
            powers = jnp.exp(scores - jnp.max(scores, axis=0, keepdims=True))
            probs = powers * (1.0 / jnp.sum(powers, axis=0, keepdims=True))
            grad_probs = dot(value, out, (1, 1))
            delta = jnp.sum(probs * grad_probs, axis=0, keepdims=True)
            score_grad = (probs * (grad_probs - delta) * scale).astype(jnp.bfloat16)
            value_grad = dot(probs.astype(jnp.bfloat16), out, (1, 0))
            key_grad = dot(score_grad, query, (1, 0))
            total += key_grad[:, NOPE:]
            query_parts.append(dot(score_grad, key, (0, 0)))
            kv_parts += [key_grad[:, :NOPE].astype(jnp.bfloat16), value_grad.astype(jnp.bfloat16)]
        rope_sum[r] = total
        q_out[r, g, :, first * QDIM : end * QDIM] = jnp.concatenate(query_parts, 1).astype(jnp.bfloat16)
        kv_out = jnp.concatenate(kv_parts, 1)
        if r == REV:
            kv_rev[g, :, first * KVDIM : end * KVDIM] = kv_out
            (kv_to_mirror(g) if end - first == heads else early_to_mirror(first)).start()
        else:
            kv_all[g, slot(my_dp), :] = kv_out
            for k in range(1, n_dp):
                kv_to_peer(g, k).start()

    def piece(ref, r, p):
        return ref.at[r, p // CUTS, pl.ds(pl.multiple_of(p % CUTS * height, height), height)]

    def query_copy(r, p):
        to = me - 1 if r == FWD else me + 1
        return remote(piece(q_out, r, p), piece(query_grad, r, p), qs_send.at[r, p], qs_recv.at[r, p], section=to)

    def to_relay(r, p):
        to = me - 2 if r == FWD else me + 2
        slot = p + my_dp * RELAYED[0]
        return remote(piece(q_out, r, p), relay_buf.at[slot], rl_send.at[r, p], rl_recv.at[slot], section=to, dp=n_dp - 1)

    def from_relay(r, d, p):
        to = me + 1 if r == FWD else me - 1
        slot = p + d * RELAYED[0]
        return remote(
            relay_buf.at[slot], piece(query_grad, r, p), rf_send.at[slot], qs_recv.at[r, p], section=to, dp=d
        )

    sends = {FWD: me > 0, REV: me < n_section - 1}
    receives = {FWD: me < n_section - 1, REV: me > 0}
    relays_out = {FWD: me == 2, REV: me == 1}
    last = my_dp == n_dp - 1
    relays_for = {FWD: (me == 0) & last, REV: (me == 3) & last}
    relay_pieces = RELAYED[0] - my_dp * (RELAYED[0] - RELAYED[1])

    def sent_directly(r, do):
        @pl.when(sends[r])
        def _():
            pl.loop(jnp.where(relays_out[r], relay_pieces, 0) if relayed else 0, groups * CUTS)(do)

    def send_queries(r):
        sent_directly(r, lambda p: query_copy(r, p).start())

    def head_copy(r, d, way):
        side = (way + 1) // 2
        ref = pieces.at[r, side, d]
        return remote(ref, ref, hp_send.at[r, side, d], hp_recv.at[r, side, d], head=my_head + way)

    def further(way, do):
        return pl.loop(my_head + 1, n_head)(do) if way > 0 else pl.loop(0, my_head)(do)

    def sum_on(way):
        side = (way + 1) // 2
        behind = has_left if way > 0 else has_right

        for r in (REV, FWD):

            def do(d):
                @pl.when(behind == 1)
                def _():
                    head_copy(r, d, way).wait_recv()
                    total = local[r, d] + pieces[r, side, d].astype(jnp.float32)
                    pieces[r, side, d] = total.astype(jnp.bfloat16)

                @pl.when(behind == 0)
                def _():
                    pieces[r, side, d] = local[r, d].astype(jnp.bfloat16)

                head_copy(r, d, way).start()

            further(way, do)

        @pl.when(behind == 1)
        def _():
            for r in (REV, FWD):
                head_copy(r, my_head, way).wait_recv()
                local[r, my_head] += pieces[r, side, my_head].astype(jnp.float32)

    def both_ways(do):
        @pl.when(my_head < n_head // 2)
        def _():
            do(1)
            do(-1)

        @pl.when(my_head >= n_head // 2)
        def _():
            do(-1)
            do(1)

    def latent_out(r):
        to = me - 1 if r == FWD else me + 1
        return remote(sums.at[r], latent_grad.at[r, 0], ls_send.at[r], ls_recv.at[r], section=to)

    keys = lax.broadcasted_iota(jnp.int32, (tokens, tokens), 0)
    at = lax.broadcasted_iota(jnp.int32, (tokens, tokens), 1)

    def run(r):
        latents_in(r)
        seg = jnp.broadcast_to(seg_buf[r], (tokens, tokens))
        allowed = (at >= keys) & (seg == jnp.transpose(seg))

        if r == REV and early:
            for first in (0, half):
                load_early(first).wait()
                compute(r, 0, allowed, first, first + half)
        else:
            compute(r, 0, allowed)

        @pl.loop(1, groups)
        def _(g):
            wait_loads(r, g)
            compute(r, g, allowed)

    load_segments.wait()
    rope_sum[...] = jnp.zeros_like(rope_sum)
    if early:
        load_queries(REV, 0).wait()
        load_out(REV, 0).wait()
    else:
        wait_loads(REV, 0)

    @pl.loop(1, groups)
    def _(g):
        start_loads(REV, g)

    load_latents(FWD).start()

    @pl.loop(0, groups)
    def _(g):
        start_loads(FWD, g)

    run(REV)
    load_latents(FWD).wait()
    for k in range(1, n_dp):
        latent_fwd(k).start()
    lt_all[my_dp] = lt_buf[FWD, pl.ds(pl.multiple_of(my_dp * rows, rows), rows), :]
    wait_loads(FWD, 0)
    run(FWD)

    send_queries(FWD)
    pl.when(me == 0)(lambda: send_queries(REV))

    for r in (REV, FWD):

        def add(g, total):
            block = kv_rev[g] if r == REV else kv_all[g, slot(my_dp), :]
            return total + dot(block, w_buf[r, g], (1, 1))

        total = lax.fori_loop(0, groups, add, jnp.zeros((tokens, latent), jnp.float32))
        local[r] = jnp.concatenate([total, rope_sum[r]], 1).reshape(n_head, mine, total.shape[1] + rope_sum.shape[2])

    both_ways(sum_on)
    for r in (REV, FWD):
        sums[r] = local[r, my_head].astype(jnp.bfloat16)

        @pl.when(sends[r])
        def _():
            latent_out(r).start()

    pl.when(me > 0)(lambda: send_queries(REV))

    zeros[...] = jnp.zeros_like(zeros)
    small_zeros[...] = jnp.zeros_like(small_zeros)
    for r in (FWD, REV):

        @pl.when(jnp.logical_not(receives[r]))
        def _():
            for copy in fill(r):
                copy.start()

    @functools.partial(holds_part, my_head)
    def _():
        for k in range(n_dp):
            latent_rev(k).wait_recv()

    def pass_on(way):
        def do(j):
            for d in range(n_dp):
                pl.when(j != my_head)(lambda: latent_part(d, j, way).wait_recv())
                pl.when((has_right if way > 0 else has_left) == 1)(lambda: latent_part(d, j, way).start())

        pass_parts(way, do)

    both_ways(pass_on)

    if early:
        early_to_mirror(0).wait_recv()
        early_to_mirror(half).wait_recv()
    else:
        kv_to_mirror(0).wait_recv()
    for k in range(1, n_dp):
        kv_passed_on(0, k).start()

    @pl.loop(1, groups)
    def _(g):
        kv_to_mirror(g).wait_recv()
        for k in range(1, n_dp):
            kv_passed_on(g, k).start()

    if relayed:
        for r in (REV, FWD):

            @pl.when(relays_out[r])
            def _():
                pl.loop(0, relay_pieces)(lambda p: to_relay(r, p).start())

    if relayed:
        for r in (REV, FWD):

            @pl.when(relays_for[r])
            def _():
                for d in range(n_dp):

                    @pl.loop(0, RELAYED[d])
                    def _(p):
                        arrived = from_relay(r, d, p)
                        remote(relay_buf.at[0], relay_buf.at[0], rf_send.at[0], rl_recv.at[p + d * RELAYED[0]]).wait_recv()
                        arrived.start()

    for k in range(1, n_dp):
        latent_fwd(k).wait_recv()
    latent_rows = jnp.concatenate([lt_all[p] for p in range(2 * n_dp)], 1)

    def put_weight(g):
        return pltpu.make_async_copy(
            w_out.at[g], weight_grad.at[0, :, pl.ds(pl.multiple_of(g * kw, 128), kw)], w_put.at[g]
        )

    @pl.loop(0, groups)
    def _(g):
        for k in range(1, n_dp):
            kv_to_peer(g, k).wait_recv()
            kv_passed_on(g, k).wait_recv()
        w_out[g] = dot(latent_rows, kv_all[g], (1, 0))
        put_weight(g).start()

    if early:
        early_to_mirror(0).wait_send()
        early_to_mirror(half).wait_send()
    else:
        kv_to_mirror(0).wait_send()

    @pl.loop(1, groups)
    def _(g):
        kv_to_mirror(g).wait_send()

    @pl.loop(0, groups)
    def _(g):
        put_weight(g).wait()
        for k in range(1, n_dp):
            kv_to_peer(g, k).wait_send()
            kv_passed_on(g, k).wait_send()

    @functools.partial(holds_part, my_head)
    def _():
        for k in range(n_dp):
            latent_rev(k).wait_send()

    for way, there in ((1, has_right), (-1, has_left)):

        @pl.when(there == 1)
        def _():
            def sent(j):
                for d in range(n_dp):
                    latent_part(d, j, way).wait_send()

            pass_parts(way, sent)

    for k in range(1, n_dp):
        latent_fwd(k).wait_send()
    for r in (REV, FWD):
        for way in (1, -1):
            further(way, lambda d: head_copy(r, d, way).wait_send())

        @pl.when(jnp.logical_not(receives[r]))
        def _():
            for copy in fill(r):
                copy.wait()

        sent_directly(r, lambda g: query_copy(r, g).wait_send())
        if relayed:

            @pl.when(relays_out[r])
            def _():
                pl.loop(0, relay_pieces)(lambda p: to_relay(r, p).wait_send())

            @pl.when(relays_for[r])
            def _():
                for d in range(n_dp):
                    pl.loop(0, RELAYED[d])(lambda p: from_relay(r, d, p).wait_send())

        @pl.when(sends[r])
        def _():
            latent_out(r).wait_send()

        @pl.when(receives[r])
        def _():
            pl.loop(0, groups * CUTS)(lambda p: query_copy(r, p).wait_recv())
            latent_out(r).wait_recv()


def relay(mesh, queries, latents, out_grad, segment_ids, up_weight):
    n_section, n_dp, n_head = (mesh.shape[a] for a in ("section", "dp", "head"))
    tokens = queries.shape[2]
    latent, width = up_weight.shape[2:]
    features = latents.shape[3]
    heads_here = width // KVDIM
    heads = next(k for k in (GROUP, 2, heads_here) if heads_here % k == 0)
    groups = heads_here // heads
    rows, mine = latent // n_dp, tokens // n_head
    kw = heads * KVDIM
    relayed = n_section == 4 and n_dp == 2 and groups * CUTS > max(RELAYED)
    slots = sum(RELAYED) if relayed else 1
    dma = pltpu.SemaphoreType.DMA
    bf16, f32 = jnp.bfloat16, jnp.float32
    anywhere = pl.BlockSpec(memory_space=pl.ANY)
    args = (queries, jnp.swapaxes(latents, 2, 3), out_grad, segment_ids, up_weight)
    flops = 2 * (2 * tokens * width * latent * 2 + 2 * tokens * tokens * heads_here * 5 * KVDIM)
    return pl.pallas_call(
        functools.partial(relay_kernel, (n_section, n_dp, n_head, heads, groups)),
        in_specs=[anywhere] * 5,
        out_specs=[anywhere] * 3,
        out_shape=[
            jax.ShapeDtypeStruct((2, groups, tokens, heads * QDIM), bf16),
            jax.ShapeDtypeStruct((2, 1, mine, features), bf16),
            jax.ShapeDtypeStruct((1, rows, width), f32),
        ],
        scratch_shapes=[
            pltpu.VMEM((2, groups, tokens, heads * QDIM), bf16),
            pltpu.VMEM((2, features, tokens), bf16),
            pltpu.VMEM((2, groups, tokens, heads * VDIM), bf16),
            pltpu.VMEM((2, groups, latent, kw), bf16),
            pltpu.VMEM((2, tokens, latent), bf16),
            pltpu.VMEM((2, tokens, features - latent), bf16),
            pltpu.VMEM((groups, tokens, kw), bf16),
            pltpu.VMEM((groups, 2 * n_dp * tokens, kw), bf16),
            pltpu.VMEM((2 * n_dp, rows, tokens), bf16),
            pltpu.VMEM((2, groups, tokens, heads * QDIM), bf16),
            pltpu.VMEM((slots, tokens // CUTS, heads * QDIM), bf16),
            pltpu.VMEM((tokens, heads * QDIM), bf16),
            pltpu.VMEM((mine, features), bf16),
            pltpu.VMEM((2, n_head, mine, features), f32),
            pltpu.VMEM((2, 2, n_head, mine, features), bf16),
            pltpu.VMEM((2, mine, features), bf16),
            pltpu.VMEM((2, tokens, features - latent), f32),
            pltpu.VMEM((groups, rows, kw), f32),
            pltpu.VMEM((2, 1, tokens), jnp.int32),
            dma((2, groups)), dma((2,)), dma((2, groups)), dma((2, groups + 1)), dma((groups,)), dma((groups + 1,)), dma,
            dma((groups + 1,)), dma((groups + 1,)), dma((groups, n_dp)), dma((groups, n_dp)),
            dma((groups, n_dp)), dma((groups, n_dp)), dma((n_dp,)), dma((n_dp,)), dma((n_dp,)), dma((n_dp,)),
            dma((n_dp, 2, n_head)), dma((n_dp, 2, n_head)),
            dma((2, groups * CUTS)), dma((2, groups * CUTS)), dma((2, groups * CUTS)), dma((slots,)), dma((slots,)), dma((2, 2, n_head)), dma((2, 2, n_head)), dma((2,)), dma((2,)),
        ],
        compiler_params=pltpu.CompilerParams(collective_id=0, has_side_effects=True, vmem_limit_bytes=44 << 20),
        cost_estimate=pl.CostEstimate(flops=flops, bytes_accessed=8 * latent * width, transcendentals=0),
        name="relay",
    )(*(pltpu.with_memory_space_constraint(x, pltpu.HBM) for x in args))


def unload_kernel(arrived, latent_in, weight_in, query_grad, latent_grad, weight_grad, sem, query_sem, weight_sem):
    groups, width = arrived.shape[1], arrived.shape[3]
    blocks = weight_sem.shape[0]
    rows = weight_in.shape[1] // blocks
    copies = (
        [
            pltpu.make_async_copy(
                weight_in.at[:, pl.ds(b * rows, rows)], weight_grad.at[:, pl.ds(b * rows, rows)], weight_sem.at[b]
            )
            for b in range(blocks)
        ]
        + [
            pltpu.make_async_copy(arrived.at[r, g], query_grad.at[r, 0, :, pl.ds(g * width, width)], query_sem.at[r, g])
            for r in (FWD, REV)
            for g in range(groups)
        ]
        + [pltpu.make_async_copy(latent_in, latent_grad, sem)]
    )
    for copy in copies:
        copy.start()
    for copy in copies:
        copy.wait()


def unload(arrived, latent_grad, weight_grad):
    two, groups, tokens, width = arrived.shape
    blocks = next(b for b in (BLOCKS, 2, 1) if weight_grad.shape[1] % (8 * b) == 0)
    anywhere = pl.BlockSpec(memory_space=pl.ANY)
    dma = pltpu.SemaphoreType.DMA
    return pl.pallas_call(
        unload_kernel,
        in_specs=[anywhere] * 3,
        out_specs=[anywhere] * 3,
        out_shape=[
            pltpu.HBM((two, 1, tokens, groups * width), arrived.dtype),
            pltpu.HBM(latent_grad.shape, latent_grad.dtype),
            pltpu.HBM(weight_grad.shape, weight_grad.dtype),
        ],
        scratch_shapes=[dma, dma((two, groups)), dma((blocks,))],
        compiler_params=pltpu.CompilerParams(vmem_limit_bytes=1 << 20),
        name="unload",
    )(arrived, latent_grad, weight_grad)


def solution(mesh):
    in_specs = (
        P(None, "section", "dp", "head"),
        P(None, "section", "dp", None),
        P(None, "section", "dp", "head"),
        P(None, "section", "dp"),
        P(None, "section", None, "head"),
    )
    out_specs = (
        P(None, "section", "dp", "head"),
        P(None, "section", ("dp", "head"), None),
        P("section", "dp", "head"),
    )
    def body(*args):
        return unload(*relay(mesh, *args))

    return jax.shard_map(body, mesh=mesh, in_specs=in_specs, out_specs=out_specs, check_vma=False)
```

```python
import functools

import jax
import jax.numpy as jnp
from jax import lax
from jax.experimental import pallas as pl
from jax.experimental.pallas import tpu as pltpu
from jax.sharding import PartitionSpec as P

ROPE = 64
NOPE = 128
VDIM = 128
QDIM = NOPE + ROPE
KVDIM = NOPE + VDIM
GROUP = 4
CUTS = 2
BLOCKS = 1
RELAYED = (6, 2)
FWD, REV = 0, 1
MESH = pl.DeviceIdType.MESH


def dot(a, b, contract):
    return lax.dot_general(a, b, ((contract[:1], contract[1:]), ((), ())), preferred_element_type=jnp.float32)


def relay_kernel(
    sizes,
    queries, latents_t, out_grad, segments, weight,
    query_grad, latent_grad, weight_grad,
    q_buf, lt_buf, o_buf, w_buf, lat, rope, kv_rev, kv_all, lt_all, q_out, relay_buf, zeros, small_zeros,
    local, pieces, sums, rope_sum, w_out, seg_buf,
    q_in, lt_in, o_in, w_in, w_put, z_put, seg_in,
    kr_send, kr_recv, kf_send, kf_recv, kx_send, kx_recv, lr_send, lr_recv, lf_send, lf_recv, lx_send, lx_recv,
    qs_send, qs_recv, rl_send, rl_recv, rf_send, hp_send, hp_recv, ls_send, ls_recv,
):
    n_section, n_dp, n_head, heads, groups = sizes
    me, my_dp, my_head = lax.axis_index("section"), lax.axis_index("dp"), lax.axis_index("head")
    mirror = n_section - 1 - me
    tokens = queries.shape[2]
    latent = weight.shape[2]
    rows = latent // n_dp
    mine = tokens // n_head
    parts = min(n_head, rows // 16)
    part = rows // parts
    kw, qw, ow = heads * KVDIM, heads * QDIM, heads * VDIM
    relayed = relay_buf.shape[0] > 1
    height = tokens // CUTS
    scale = QDIM ** (-0.5)

    def remote(src, dst, send, recv, **where):
        return pltpu.make_async_remote_copy(
            src_ref=src, dst_ref=dst, send_sem=send, recv_sem=recv, device_id=where, device_id_type=MESH
        )

    def dp_peer(k):
        return lax.rem(my_dp + k, n_dp)

    def load_weight(r, g):
        cols = pl.ds(pl.multiple_of(g * kw, 128), kw)
        return pltpu.make_async_copy(weight.at[r, 0, :, cols], w_buf.at[r, g], w_in.at[r, g])

    half = heads // 2
    early = heads % 4 == 0

    def load_early(first):
        cols = pl.ds(first * KVDIM, half * KVDIM)
        return pltpu.make_async_copy(
            weight.at[REV, 0, :, cols], w_buf.at[REV, 0, :, cols], w_in.at[REV, groups * min(first, 1)]
        )

    def load_latents(r):
        return pltpu.make_async_copy(latents_t.at[r, 0], lt_buf.at[r], lt_in.at[r])

    def load_queries(r, g):
        cols = pl.ds(pl.multiple_of(g * qw, 128), qw)
        return pltpu.make_async_copy(queries.at[r, 0, :, cols], q_buf.at[r, g], q_in.at[r, g])

    def load_out(r, g):
        cols = pl.ds(pl.multiple_of(g * ow, 128), ow)
        return pltpu.make_async_copy(out_grad.at[r, 0, :, cols], o_buf.at[r, g], o_in.at[r, g])

    def start_loads(r, g):
        load_weight(r, g).start()
        load_queries(r, g).start()
        load_out(r, g).start()

    def wait_loads(r, g):
        load_weight(r, g).wait()
        load_queries(r, g).wait()
        load_out(r, g).wait()

    has_left, has_right = jnp.where(my_head > 0, 1, 0), jnp.where(my_head < n_head - 1, 1, 0)
    barrier = pltpu.get_barrier_semaphore()
    for k in range(1, n_section):
        pl.semaphore_signal(barrier, 1, device_id={"section": lax.rem(me + k, n_section)}, device_id_type=MESH)
    for k in range(1, n_dp):
        pl.semaphore_signal(barrier, 1, device_id={"dp": dp_peer(k)}, device_id_type=MESH)
        for section in [lax.rem(me + j, n_section) for j in range(1, n_section)] if relayed else [mirror]:
            pl.semaphore_signal(barrier, 1, device_id={"section": section, "dp": dp_peer(k)}, device_id_type=MESH)
    for step in (-1, 1):

        @pl.when((my_head + step >= 0) & (my_head + step < n_head))
        def _():
            pl.semaphore_signal(barrier, 1, device_id={"head": my_head + step}, device_id_type=MESH)


    load_segments = pltpu.make_async_copy(segments, seg_buf, seg_in)
    load_latents(REV).start()
    load_segments.start()
    if early:
        load_early(0).start()
        load_queries(REV, 0).start()
        load_out(REV, 0).start()
        load_early(half).start()
    else:
        start_loads(REV, 0)

    def latents_in(r):
        lat[r] = jnp.transpose(lt_buf[r, :latent, :].astype(jnp.float32)).astype(jnp.bfloat16)
        rope[r] = jnp.transpose(lt_buf[r, latent:, :].astype(jnp.float32)).astype(jnp.bfloat16)

    load_latents(REV).wait()
    pl.semaphore_wait(barrier, n_section - 1 + (n_section if relayed else 2) * (n_dp - 1) + has_left + has_right)

    def latent_rev(k):
        to = dp_peer(k)
        block = pl.ds(pl.multiple_of(to * rows + my_head * part, part), part)
        return remote(
            lt_buf.at[REV, block],
            lt_all.at[n_dp + my_dp, pl.ds(pl.multiple_of(my_head * part, part), part)],
            lr_send.at[k],
            lr_recv.at[k],
            section=mirror,
            dp=to,
        )

    def latent_fwd(k):
        to = dp_peer(k)
        block = pl.ds(pl.multiple_of(to * rows, rows), rows)
        return remote(lt_buf.at[FWD, block], lt_all.at[my_dp], lf_send.at[k], lf_recv.at[k], dp=to)

    def latent_part(d, j, way):
        ref = lt_all.at[n_dp + d, pl.ds(pl.multiple_of(j * part, part), part)]
        side = (way + 1) // 2
        return remote(ref, ref, lx_send.at[d, side, j], lx_recv.at[d, side, j], head=my_head + way)

    def pass_parts(way, do):
        low, high = (0, jnp.minimum(my_head + 1, parts)) if way > 0 else (my_head, parts)
        return pl.loop(low, high)(do)

    def holds_part(head, do):
        if parts == n_head:
            do()
        else:
            pl.when(head < parts)(do)

    @functools.partial(holds_part, my_head)
    def _():
        for k in range(n_dp):
            latent_rev(k).start()

    def fill(r):
        return [
            pltpu.make_async_copy(zeros, query_grad.at[r, g], z_put.at[g]) for g in range(groups)
        ] + [pltpu.make_async_copy(small_zeros, latent_grad.at[r, 0], z_put.at[groups])]

    def slot(piece):
        return pl.ds(pl.multiple_of(piece * tokens, tokens), tokens)

    def kv_to_mirror(g):
        return remote(kv_rev.at[g], kv_all.at[g, slot(n_dp + my_dp)], kr_send.at[g], kr_recv.at[g], section=mirror)

    def early_to_mirror(first):
        cols, sem = pl.ds(first * KVDIM, half * KVDIM), groups * min(first, 1)
        return remote(
            kv_rev.at[0, :, cols], kv_all.at[0, slot(n_dp + my_dp), cols], kr_send.at[sem], kr_recv.at[sem], section=mirror
        )

    def kv_to_peer(g, k):
        ref = kv_all.at[g, slot(my_dp)]
        return remote(ref, ref, kf_send.at[g, k], kf_recv.at[g, k], dp=dp_peer(k))

    def kv_passed_on(g, k):
        ref = kv_all.at[g, slot(n_dp + my_dp)]
        return remote(ref, ref, kx_send.at[g, k], kx_recv.at[g, k], dp=dp_peer(k))

    def compute(r, g, allowed, first=0, end=heads):
        kv = dot(lat[r], w_buf[r, g, :, first * KVDIM : end * KVDIM], (1, 0)).astype(jnp.bfloat16)
        query_block = q_buf[r, g, :, first * QDIM : end * QDIM]
        out_block = o_buf[r, g, :, first * VDIM : end * VDIM]
        key_rope = rope[r]
        query_parts, kv_parts = [], []
        total = rope_sum[r]
        for h in range(end - first):
            key = jnp.concatenate([kv[:, h * KVDIM : h * KVDIM + NOPE], key_rope], 1)
            value = kv[:, h * KVDIM + NOPE : (h + 1) * KVDIM]
            query = query_block[:, h * QDIM : (h + 1) * QDIM]
            out = out_block[:, h * VDIM : (h + 1) * VDIM]
            scores = jnp.where(allowed, dot(key, query, (1, 1)) * scale, jnp.float32(-1e30))
            powers = jnp.exp(scores - jnp.max(scores, axis=0, keepdims=True))
            probs = powers * (1.0 / jnp.sum(powers, axis=0, keepdims=True))
            grad_probs = dot(value, out, (1, 1))
            delta = jnp.sum(probs * grad_probs, axis=0, keepdims=True)
            score_grad = (probs * (grad_probs - delta) * scale).astype(jnp.bfloat16)
            value_grad = dot(probs.astype(jnp.bfloat16), out, (1, 0))
            key_grad = dot(score_grad, query, (1, 0))
            total += key_grad[:, NOPE:]
            query_parts.append(dot(score_grad, key, (0, 0)))
            kv_parts += [key_grad[:, :NOPE].astype(jnp.bfloat16), value_grad.astype(jnp.bfloat16)]
        rope_sum[r] = total
        q_out[r, g, :, first * QDIM : end * QDIM] = jnp.concatenate(query_parts, 1).astype(jnp.bfloat16)
        kv_out = jnp.concatenate(kv_parts, 1)
        if r == REV:
            kv_rev[g, :, first * KVDIM : end * KVDIM] = kv_out
            (kv_to_mirror(g) if end - first == heads else early_to_mirror(first)).start()
        else:
            kv_all[g, slot(my_dp), :] = kv_out
            for k in range(1, n_dp):
                kv_to_peer(g, k).start()

    def piece(ref, r, p):
        return ref.at[r, p // CUTS, pl.ds(pl.multiple_of(p % CUTS * height, height), height)]

    def query_copy(r, p):
        to = me - 1 if r == FWD else me + 1
        return remote(piece(q_out, r, p), piece(query_grad, r, p), qs_send.at[r, p], qs_recv.at[r, p], section=to)

    def to_relay(r, p):
        to = me - 2 if r == FWD else me + 2
        slot = p + my_dp * RELAYED[0]
        return remote(piece(q_out, r, p), relay_buf.at[slot], rl_send.at[r, p], rl_recv.at[slot], section=to, dp=n_dp - 1)

    def from_relay(r, d, p):
        to = me + 1 if r == FWD else me - 1
        slot = p + d * RELAYED[0]
        return remote(
            relay_buf.at[slot], piece(query_grad, r, p), rf_send.at[slot], qs_recv.at[r, p], section=to, dp=d
        )

    sends = {FWD: me > 0, REV: me < n_section - 1}
    receives = {FWD: me < n_section - 1, REV: me > 0}
    relays_out = {FWD: me == 2, REV: me == 1}
    last = my_dp == n_dp - 1
    relays_for = {FWD: (me == 0) & last, REV: (me == 3) & last}
    relay_pieces = RELAYED[0] - my_dp * (RELAYED[0] - RELAYED[1])

    def group_copy(r, g):
        to = me - 1 if r == FWD else me + 1
        sem = g * CUTS
        return remote(q_out.at[r, g], query_grad.at[r, g], qs_send.at[r, sem], qs_recv.at[r, sem], section=to)

    def each_copy(r, active, in_pieces, first, do):
        @pl.when(active & jnp.logical_not(in_pieces) if relayed else active)
        def _():
            pl.loop(0, groups)(lambda g: do(group_copy(r, g)))

        if relayed:

            @pl.when(in_pieces)
            def _():
                pl.loop(first, groups * CUTS)(lambda p: do(query_copy(r, p)))

    def sent_directly(r, do):
        each_copy(r, sends[r], relays_out[r], relay_pieces, do)

    def send_queries(r):
        sent_directly(r, lambda copy: copy.start())

    def head_copy(r, d, way):
        side = (way + 1) // 2
        ref = pieces.at[r, side, d]
        return remote(ref, ref, hp_send.at[r, side, d], hp_recv.at[r, side, d], head=my_head + way)

    def further(way, do):
        return pl.loop(my_head + 1, n_head)(do) if way > 0 else pl.loop(0, my_head)(do)

    def sum_on(way):
        side = (way + 1) // 2
        behind = has_left if way > 0 else has_right

        for r in (REV, FWD):

            def do(d):
                @pl.when(behind == 1)
                def _():
                    head_copy(r, d, way).wait_recv()
                    total = local[r, d] + pieces[r, side, d].astype(jnp.float32)
                    pieces[r, side, d] = total.astype(jnp.bfloat16)

                @pl.when(behind == 0)
                def _():
                    pieces[r, side, d] = local[r, d].astype(jnp.bfloat16)

                head_copy(r, d, way).start()

            further(way, do)

        @pl.when(behind == 1)
        def _():
            for r in (REV, FWD):
                head_copy(r, my_head, way).wait_recv()
                local[r, my_head] += pieces[r, side, my_head].astype(jnp.float32)

    def both_ways(do):
        @pl.when(my_head < n_head // 2)
        def _():
            do(1)
            do(-1)

        @pl.when(my_head >= n_head // 2)
        def _():
            do(-1)
            do(1)

    def latent_out(r):
        to = me - 1 if r == FWD else me + 1
        return remote(sums.at[r], latent_grad.at[r, 0], ls_send.at[r], ls_recv.at[r], section=to)

    keys = lax.broadcasted_iota(jnp.int32, (tokens, tokens), 0)
    at = lax.broadcasted_iota(jnp.int32, (tokens, tokens), 1)

    def run(r):
        latents_in(r)
        seg = jnp.broadcast_to(seg_buf[r], (tokens, tokens))
        allowed = (at >= keys) & (seg == jnp.transpose(seg))

        if r == REV and early:
            for first in (0, half):
                load_early(first).wait()
                compute(r, 0, allowed, first, first + half)
        else:
            compute(r, 0, allowed)

        @pl.loop(1, groups)
        def _(g):
            wait_loads(r, g)
            compute(r, g, allowed)

    load_segments.wait()
    rope_sum[...] = jnp.zeros_like(rope_sum)
    if early:
        load_queries(REV, 0).wait()
        load_out(REV, 0).wait()
    else:
        wait_loads(REV, 0)

    @pl.loop(1, groups)
    def _(g):
        start_loads(REV, g)

    load_latents(FWD).start()

    @pl.loop(0, groups)
    def _(g):
        start_loads(FWD, g)

    run(REV)
    load_latents(FWD).wait()
    for k in range(1, n_dp):
        latent_fwd(k).start()
    lt_all[my_dp] = lt_buf[FWD, pl.ds(pl.multiple_of(my_dp * rows, rows), rows), :]
    wait_loads(FWD, 0)
    run(FWD)

    send_queries(FWD)
    pl.when(me == 0)(lambda: send_queries(REV))

    for r in (REV, FWD):

        def add(g, total):
            block = kv_rev[g] if r == REV else kv_all[g, slot(my_dp), :]
            return total + dot(block, w_buf[r, g], (1, 1))

        total = lax.fori_loop(0, groups, add, jnp.zeros((tokens, latent), jnp.float32))
        local[r] = jnp.concatenate([total, rope_sum[r]], 1).reshape(n_head, mine, total.shape[1] + rope_sum.shape[2])

    both_ways(sum_on)
    for r in (REV, FWD):
        sums[r] = local[r, my_head].astype(jnp.bfloat16)

        @pl.when(sends[r])
        def _():
            latent_out(r).start()

    pl.when(me > 0)(lambda: send_queries(REV))

    zeros[...] = jnp.zeros_like(zeros)
    small_zeros[...] = jnp.zeros_like(small_zeros)
    for r in (FWD, REV):

        @pl.when(jnp.logical_not(receives[r]))
        def _():
            for copy in fill(r):
                copy.start()

    @functools.partial(holds_part, my_head)
    def _():
        for k in range(n_dp):
            latent_rev(k).wait_recv()

    def pass_on(way):
        def do(j):
            for d in range(n_dp):
                pl.when(j != my_head)(lambda: latent_part(d, j, way).wait_recv())
                pl.when((has_right if way > 0 else has_left) == 1)(lambda: latent_part(d, j, way).start())

        pass_parts(way, do)

    both_ways(pass_on)

    if early:
        early_to_mirror(0).wait_recv()
        early_to_mirror(half).wait_recv()
    else:
        kv_to_mirror(0).wait_recv()
    for k in range(1, n_dp):
        kv_passed_on(0, k).start()

    @pl.loop(1, groups)
    def _(g):
        kv_to_mirror(g).wait_recv()
        for k in range(1, n_dp):
            kv_passed_on(g, k).start()

    if relayed:
        for r in (REV, FWD):

            @pl.when(relays_out[r])
            def _():
                pl.loop(0, relay_pieces)(lambda p: to_relay(r, p).start())

    if relayed:
        for r in (REV, FWD):

            @pl.when(relays_for[r])
            def _():
                for d in range(n_dp):

                    @pl.loop(0, RELAYED[d])
                    def _(p):
                        arrived = from_relay(r, d, p)
                        remote(relay_buf.at[0], relay_buf.at[0], rf_send.at[0], rl_recv.at[p + d * RELAYED[0]]).wait_recv()
                        arrived.start()

    for k in range(1, n_dp):
        latent_fwd(k).wait_recv()
    latent_rows = jnp.concatenate([lt_all[p] for p in range(2 * n_dp)], 1)

    def put_weight(g):
        return pltpu.make_async_copy(
            w_out.at[g], weight_grad.at[0, :, pl.ds(pl.multiple_of(g * kw, 128), kw)], w_put.at[g]
        )

    @pl.loop(0, groups)
    def _(g):
        for k in range(1, n_dp):
            kv_to_peer(g, k).wait_recv()
            kv_passed_on(g, k).wait_recv()
        w_out[g] = dot(latent_rows, kv_all[g], (1, 0))
        put_weight(g).start()

    if early:
        early_to_mirror(0).wait_send()
        early_to_mirror(half).wait_send()
    else:
        kv_to_mirror(0).wait_send()

    @pl.loop(1, groups)
    def _(g):
        kv_to_mirror(g).wait_send()

    @pl.loop(0, groups)
    def _(g):
        put_weight(g).wait()
        for k in range(1, n_dp):
            kv_to_peer(g, k).wait_send()
            kv_passed_on(g, k).wait_send()

    @functools.partial(holds_part, my_head)
    def _():
        for k in range(n_dp):
            latent_rev(k).wait_send()

    for way, there in ((1, has_right), (-1, has_left)):

        @pl.when(there == 1)
        def _():
            def sent(j):
                for d in range(n_dp):
                    latent_part(d, j, way).wait_send()

            pass_parts(way, sent)

    for k in range(1, n_dp):
        latent_fwd(k).wait_send()
    for r in (REV, FWD):
        for way in (1, -1):
            further(way, lambda d: head_copy(r, d, way).wait_send())

        @pl.when(jnp.logical_not(receives[r]))
        def _():
            for copy in fill(r):
                copy.wait()

        sent_directly(r, lambda copy: copy.wait_send())
        if relayed:

            @pl.when(relays_out[r])
            def _():
                pl.loop(0, relay_pieces)(lambda p: to_relay(r, p).wait_send())

            @pl.when(relays_for[r])
            def _():
                for d in range(n_dp):
                    pl.loop(0, RELAYED[d])(lambda p: from_relay(r, d, p).wait_send())

        @pl.when(sends[r])
        def _():
            latent_out(r).wait_send()

        @pl.when(receives[r])
        def _():
            latent_out(r).wait_recv()

        each_copy(r, receives[r], me == (1 if r == FWD else 2), 0, lambda copy: copy.wait_recv())


def relay(mesh, queries, latents, out_grad, segment_ids, up_weight):
    n_section, n_dp, n_head = (mesh.shape[a] for a in ("section", "dp", "head"))
    tokens = queries.shape[2]
    latent, width = up_weight.shape[2:]
    features = latents.shape[3]
    heads_here = width // KVDIM
    heads = next(k for k in (GROUP, 2, heads_here) if heads_here % k == 0)
    groups = heads_here // heads
    rows, mine = latent // n_dp, tokens // n_head
    kw = heads * KVDIM
    relayed = n_section == 4 and n_dp == 2 and groups * CUTS > max(RELAYED)
    slots = sum(RELAYED) if relayed else 1
    dma = pltpu.SemaphoreType.DMA
    bf16, f32 = jnp.bfloat16, jnp.float32
    anywhere = pl.BlockSpec(memory_space=pl.ANY)
    args = (queries, jnp.swapaxes(latents, 2, 3), out_grad, segment_ids, up_weight)
    flops = 2 * (2 * tokens * width * latent * 2 + 2 * tokens * tokens * heads_here * 5 * KVDIM)
    return pl.pallas_call(
        functools.partial(relay_kernel, (n_section, n_dp, n_head, heads, groups)),
        in_specs=[anywhere] * 5,
        out_specs=[anywhere] * 3,
        out_shape=[
            jax.ShapeDtypeStruct((2, groups, tokens, heads * QDIM), bf16),
            jax.ShapeDtypeStruct((2, 1, mine, features), bf16),
            jax.ShapeDtypeStruct((1, rows, width), f32),
        ],
        scratch_shapes=[
            pltpu.VMEM((2, groups, tokens, heads * QDIM), bf16),
            pltpu.VMEM((2, features, tokens), bf16),
            pltpu.VMEM((2, groups, tokens, heads * VDIM), bf16),
            pltpu.VMEM((2, groups, latent, kw), bf16),
            pltpu.VMEM((2, tokens, latent), bf16),
            pltpu.VMEM((2, tokens, features - latent), bf16),
            pltpu.VMEM((groups, tokens, kw), bf16),
            pltpu.VMEM((groups, 2 * n_dp * tokens, kw), bf16),
            pltpu.VMEM((2 * n_dp, rows, tokens), bf16),
            pltpu.VMEM((2, groups, tokens, heads * QDIM), bf16),
            pltpu.VMEM((slots, tokens // CUTS, heads * QDIM), bf16),
            pltpu.VMEM((tokens, heads * QDIM), bf16),
            pltpu.VMEM((mine, features), bf16),
            pltpu.VMEM((2, n_head, mine, features), f32),
            pltpu.VMEM((2, 2, n_head, mine, features), bf16),
            pltpu.VMEM((2, mine, features), bf16),
            pltpu.VMEM((2, tokens, features - latent), f32),
            pltpu.VMEM((groups, rows, kw), f32),
            pltpu.VMEM((2, 1, tokens), jnp.int32),
            dma((2, groups)), dma((2,)), dma((2, groups)), dma((2, groups + 1)), dma((groups,)), dma((groups + 1,)), dma,
            dma((groups + 1,)), dma((groups + 1,)), dma((groups, n_dp)), dma((groups, n_dp)),
            dma((groups, n_dp)), dma((groups, n_dp)), dma((n_dp,)), dma((n_dp,)), dma((n_dp,)), dma((n_dp,)),
            dma((n_dp, 2, n_head)), dma((n_dp, 2, n_head)),
            dma((2, groups * CUTS)), dma((2, groups * CUTS)), dma((2, groups * CUTS)), dma((slots,)), dma((slots,)), dma((2, 2, n_head)), dma((2, 2, n_head)), dma((2,)), dma((2,)),
        ],
        compiler_params=pltpu.CompilerParams(collective_id=0, has_side_effects=True, vmem_limit_bytes=44 << 20),
        cost_estimate=pl.CostEstimate(flops=flops, bytes_accessed=8 * latent * width, transcendentals=0),
        name="relay",
    )(*(pltpu.with_memory_space_constraint(x, pltpu.HBM) for x in args))


def unload_kernel(arrived, latent_in, weight_in, query_grad, latent_grad, weight_grad, sem, query_sem, weight_sem):
    groups, width = arrived.shape[1], arrived.shape[3]
    blocks = weight_sem.shape[0]
    rows = weight_in.shape[1] // blocks
    copies = (
        [
            pltpu.make_async_copy(
                weight_in.at[:, pl.ds(b * rows, rows)], weight_grad.at[:, pl.ds(b * rows, rows)], weight_sem.at[b]
            )
            for b in range(blocks)
        ]
        + [
            pltpu.make_async_copy(arrived.at[r, g], query_grad.at[r, 0, :, pl.ds(g * width, width)], query_sem.at[r, g])
            for r in (FWD, REV)
            for g in range(groups)
        ]
        + [pltpu.make_async_copy(latent_in, latent_grad, sem)]
    )
    for copy in copies:
        copy.start()
    for copy in copies:
        copy.wait()


def unload(arrived, latent_grad, weight_grad):
    two, groups, tokens, width = arrived.shape
    blocks = next(b for b in (BLOCKS, 2, 1) if weight_grad.shape[1] % (8 * b) == 0)
    anywhere = pl.BlockSpec(memory_space=pl.ANY)
    dma = pltpu.SemaphoreType.DMA
    return pl.pallas_call(
        unload_kernel,
        in_specs=[anywhere] * 3,
        out_specs=[anywhere] * 3,
        out_shape=[
            pltpu.HBM((two, 1, tokens, groups * width), arrived.dtype),
            pltpu.HBM(latent_grad.shape, latent_grad.dtype),
            pltpu.HBM(weight_grad.shape, weight_grad.dtype),
        ],
        scratch_shapes=[dma, dma((two, groups)), dma((blocks,))],
        compiler_params=pltpu.CompilerParams(vmem_limit_bytes=1 << 20),
        name="unload",
    )(arrived, latent_grad, weight_grad)


def solution(mesh):
    in_specs = (
        P(None, "section", "dp", "head"),
        P(None, "section", "dp", None),
        P(None, "section", "dp", "head"),
        P(None, "section", "dp"),
        P(None, "section", None, "head"),
    )
    out_specs = (
        P(None, "section", "dp", "head"),
        P(None, "section", ("dp", "head"), None),
        P("section", "dp", "head"),
    )
    def body(*args):
        return unload(*relay(mesh, *args))

    return jax.shard_map(body, mesh=mesh, in_specs=in_specs, out_specs=out_specs, check_vma=False)
```
